32 devices in a mesh: harm: 8 (over z, y), node: 4 (over x, core).
Axes of the slice: x: 2, y: 2, z: 4, core: 2. Of those that a mesh axis runs over, the one named last changes fastest.
Arguments:
- state: float32 [2, 128, 64, 128], P(None, 'harm', 'node'), may hold values from -0.6 to 0.6
- source: float32 [2, 128, 64, 128], P(None, 'harm', 'node'), may hold values from -6 to 6
- capacity: float32 [64, 128], P('node'), may hold values from 0.05 to 0.5
- row_shift: int32 [64], P('node'), may hold values from 0 to 3
- device_type: int32 [64, 128], P('node'), may hold values from 0 to 3
- device_table: float32 [3, 4], replicated, may hold values from 0.5 to 2
- precond: float32 [2, 128, 128, 128], P(None, 'harm'), may hold values from -1 to 1, as said below
Outputs:
- update: float32 [2, 128, 64, 128], P(None, 'harm', 'node')
- resid: float32 [2, 128, 64, 128], P(None, 'harm', 'node')
The draws below stay inside these ranges and needn't reach their ends.
Inputs may be any that keep to these rules, and one draw needn't show every extreme that they name: precond[0, k] is 1/6 on the diagonal plus a full-rank fluctuation; precond[1, k] is a full-rank fluctuation.
All inputs are finite; a program needn't handle non-finite values.
Results may differ from the reference program's by a relative error of at most 0.00011.
Values sent between devices are 32-bit elements; how exact they have to be, the bound alone decides.
A program may use at most 64 MiB of HBM per device.

```python
import math
import jax
import jax.numpy as jnp
from jax import lax

H = 128
S = 256
GY = 128
ITERS = 3
TYPES = 4
SHIFTS = 4
GX = 64


def draw_precond(key, part):
    first_key, second_key = jax.random.split(jax.random.fold_in(key, 17))
    noise_real = jnp.clip(jax.random.normal(first_key, (H, GY, GY), jnp.float32), -4.0, 4.0)
    noise_imag = jnp.clip(jax.random.normal(second_key, (H, GY, GY), jnp.float32), -4.0, 4.0)
    identity = jnp.eye(GY, dtype=jnp.float32)[None]
    real_part = (identity + 0.5 * noise_real / jnp.sqrt(GY * 1.0)) / 6.0
    imag_part = 0.5 * noise_imag / jnp.sqrt(GY * 1.0) / 6.0
    return jnp.stack([real_part, imag_part])


def set_ends(values, key, low, top_value):
    longest = values.shape.index(max(values.shape))
    spots = []
    for shift in (0, 1):
        where = [jax.random.randint(jax.random.fold_in(key, axis), (), 0, length) for axis, length in enumerate(values.shape)]
        where[longest] = (where[longest] + shift) % values.shape[longest]
        spots.append(tuple(where))
    return values.at[spots[0]].set(low).at[spots[1]].set(top_value)


def block_levels(stream_key, extent, cuts, low, largest):
    loudness = 1.0
    for axis_at, blocks in cuts:
        draws = jax.random.uniform(jax.random.fold_in(jax.random.fold_in(stream_key, 6), axis_at), (blocks,), jnp.float32, low / len(cuts), largest / len(cuts))
        loudness = loudness * jnp.repeat(jnp.exp(draws), extent[axis_at] // blocks).reshape((-1,) + (1,) * (len(extent) - 1 - axis_at))
    return loudness


def normal_values(key, shape, deviation, most, pieces=(), kind=jnp.bfloat16):
    values = deviation * jax.random.normal(key, shape, jnp.float32)
    if pieces:
        values = values * block_levels(key, shape, pieces, -0.22, 0.18)
    return jnp.clip(values, -most, most).astype(kind)


def setup_inputs(seed: int = 0) -> dict:
    keys = jax.random.split(jax.random.key(seed), 8)
    return {
        "state": normal_values(keys[0], (2, H, GX, GY), 0.1, 0.6, ((1, 8), (2, 4)), jnp.float32),
        "source": normal_values(keys[1], (2, H, GX, GY), 1.0, 6.0, ((1, 8), (2, 4)), jnp.float32),
        "capacity": jnp.clip(jnp.exp(math.log(0.5) - 2.3025851 * jax.random.uniform(keys[2], (GX, GY), jnp.float32) ** block_levels(keys[2], (GX, GY), ((0, 4),), -0.2, 0.2)), 0.05, 0.5),
        "row_shift": set_ends(jax.random.randint(keys[3], (GX,), 0, SHIFTS), jax.random.fold_in(keys[3], 1), 0, SHIFTS - 1).astype(jnp.int32),
        "device_type": set_ends(jax.random.randint(keys[4], (GX, GY), 0, TYPES), jax.random.fold_in(keys[4], 1), 0, TYPES - 1).astype(jnp.int32),
        "device_table": jnp.clip(jax.random.uniform(keys[5], (3, TYPES), jnp.float32, 0.5, 2.0), 0.5, 2.0),
        "precond": draw_precond(jax.random.fold_in(keys[7], 71), 0),
    }


omega_step = 0.05
top = lax.Precision.HIGHEST

def small_solve(gram, right):
    lower = jnp.linalg.cholesky(gram)
    order = gram.shape[0]
    forward = []
    for column in range(order):
        value = right[column]
        for member in range(column):
            value = value - lower[column, member] * forward[member]
        forward.append(value / lower[column, column])
    result = [None] * order
    for column in reversed(range(order)):
        value = forward[column]
        for member in range(column + 1, order):
            value = value - lower[member, column] * result[member]
        result[column] = value / lower[column, column]
    return result

def weights_of():
    waves = jnp.arange(H)
    return jnp.where(waves == 0, 1.0, 2.0).astype(jnp.float32)

def to_time(spectrum):
    scaled = (spectrum[0] + 1j * spectrum[1]) * (S / weights_of())[:, None, None]
    padded = jnp.concatenate([scaled, jnp.zeros((1,) + scaled.shape[1:], scaled.dtype)], axis=0)
    return jnp.fft.irfft(padded, n=S, axis=0)

def to_spec(signal):
    trans = jnp.fft.rfft(signal, axis=0)[:H]
    factor = (weights_of() / S)[:, None, None]
    return jnp.stack([jnp.real(trans) * factor, jnp.imag(trans) * factor])

def stencil(field, capacity, row_shift):
    left_side = jnp.roll(field, 1, axis=3)
    right_side = jnp.roll(field, -1, axis=3)
    zero_row = jnp.zeros(field.shape[:2] + (1, field.shape[3]), jnp.float32)
    above = jnp.concatenate([zero_row, field[:, :, :-1]], axis=2)
    below = jnp.concatenate([field[:, :, 1:], zero_row], axis=2)
    skewed = jnp.zeros_like(field)
    for amount in range(SHIFTS):
        picked = (row_shift == amount).astype(jnp.float32)[None, None, :, None]
        skewed = skewed + picked * jnp.roll(above, -amount, axis=3)
    result = 4.0 * field - left_side - right_side - skewed - below
    waves = jnp.arange(H).astype(jnp.float32)
    reactive = omega_step * waves[:, None, None] * capacity[None]
    return result + jnp.stack([-reactive * field[1], reactive * field[0]])

def precondition(field, blocks):
    real_part = jnp.einsum('krd,kcd->krc', field[0], blocks[0], precision=top) - jnp.einsum('krd,kcd->krc', field[1], blocks[1], precision=top)
    imag_part = jnp.einsum('krd,kcd->krc', field[0], blocks[1], precision=top) + jnp.einsum('krd,kcd->krc', field[1], blocks[0], precision=top)
    return jnp.stack([real_part, imag_part])

def reference(state, source, capacity, row_shift, device_type, device_table, precond):
    params = jnp.zeros((3,) + device_type.shape, jnp.float32)
    for member in range(TYPES):
        params = params + (device_type == member).astype(jnp.float32)[None] * device_table[:, member][:, None, None]
    linear, amplitude, slope = (params[0], params[1], params[2])
    voltage = to_time(state)
    bent = jnp.tanh(slope * voltage)
    flow = linear * voltage + amplitude * bent
    slopes = linear + amplitude * slope * (1.0 - bent * bent)
    resid = stencil(state, capacity, row_shift) + to_spec(flow) - source
    start = -resid
    beta = jnp.sqrt(jnp.sum(start * start))
    basis = [start / beta]
    directions = []
    columns_h = []
    for iteration in range(ITERS):
        direction = precondition(basis[iteration], precond)
        directions.append(direction)
        image = stencil(direction, capacity, row_shift) + to_spec(slopes * to_time(direction))
        heights = []
        for earlier in range(iteration + 1):
            height = jnp.sum(basis[earlier] * image)
            image = image - height * basis[earlier]
            heights.append(height)
        length = jnp.sqrt(jnp.sum(image * image))
        columns_h.append(jnp.stack(heights + [length] + [jnp.zeros((), jnp.float32)] * (ITERS - 1 - iteration)))
        if iteration + 1 < ITERS:
            basis.append(image / length)
    hess = jnp.stack(columns_h, axis=1)
    gram = jnp.dot(hess.T, hess, precision=top)
    coeffs = small_solve(gram, beta * hess[0])
    update = jnp.zeros_like(state)
    for iteration in range(ITERS):
        update = update + coeffs[iteration] * directions[iteration]
    return (update, resid)
```

```python
import functools

import jax
import jax.numpy as jnp
import numpy as np
from jax import lax
from jax.experimental import pallas as pl
from jax.experimental.pallas import tpu as pltpu
from jax.sharding import PartitionSpec as P

ITERS = 3
TYPES = 4
SHIFTS = 4


omega_step = 0.05
top = lax.Precision.HIGHEST


def extended(cells, sides, width):
    for axis, dim in sides:
        count = lax.axis_size(axis)
        ends = count - 1
        head = lax.slice_in_dim(cells, 0, width, axis=dim)
        tail = lax.slice_in_dim(cells, cells.shape[dim] - width, cells.shape[dim], axis=dim)
        cells = jnp.concatenate(
            [
                lax.ppermute(tail, axis, [(i, (i + 1) % count) for i in range(ends)]),
                cells,
                lax.ppermute(head, axis, [((i + 1) % count, i) for i in range(ends)]),
            ],
            axis=dim,
        )
    return cells


def small_solve(gram, right):
    lower = jnp.linalg.cholesky(gram)
    order = gram.shape[0]
    forward = []
    for column in range(order):
        value = right[column]
        for member in range(column):
            value = value - lower[column, member] * forward[member]
        forward.append(value / lower[column, column])
    result = [None] * order
    for column in reversed(range(order)):
        value = forward[column]
        for member in range(column + 1, order):
            value = value - lower[member, column] * result[member]
        result[column] = value / lower[column, column]
    return result


def tables(harmonics, samples):
    waves = jnp.arange(harmonics, dtype=jnp.int32)
    moments = jnp.arange(samples, dtype=jnp.int32)
    phase = (moments[:, None] * waves[None, :] % samples).astype(jnp.float32) * (
        2.0 * jnp.pi / samples
    )
    cosine = jnp.cos(phase)
    sine = jnp.sin(phase)
    inverse = jnp.concatenate([cosine, -sine], axis=1)
    weights = jnp.where(waves == 0, 1.0, 2.0).astype(jnp.float32) / samples
    forward = jnp.concatenate([cosine.T * weights[:, None], -sine.T * weights[:, None]], axis=0)
    return (inverse, forward)


def stencil(field, above, below, capacity, shifts, waves):
    left_side = jnp.roll(field, 1, axis=3)
    right_side = jnp.roll(field, -1, axis=3)
    skewed = jnp.zeros_like(field)
    for amount in range(SHIFTS):
        picked = (shifts == amount).astype(jnp.float32)[None, None, :, None]
        skewed = skewed + picked * jnp.roll(above, -amount, axis=3)
    result = 4.0 * field - left_side - right_side - skewed - below
    reactive = omega_step * waves.astype(jnp.float32)[:, None, None] * capacity[None]
    return result + jnp.stack([-reactive * field[1], reactive * field[0]])


def precondition(field, blocks):
    real_part = jnp.einsum("krd,kcd->krc", field[0], blocks[0], precision=top) - jnp.einsum(
        "krd,kcd->krc", field[1], blocks[1], precision=top
    )
    imag_part = jnp.einsum("krd,kcd->krc", field[0], blocks[1], precision=top) + jnp.einsum(
        "krd,kcd->krc", field[1], blocks[0], precision=top
    )
    return jnp.stack([real_part, imag_part])


def body(state, source, capacity, row_shift, device_type, device_table, precond):
    groups = lax.axis_size("harm")
    place = lax.axis_index("harm")
    local_harm = state.shape[1]
    block_rows = state.shape[2]
    columns = state.shape[3]
    harmonics = local_harm * groups
    samples = 2 * harmonics
    own_rows = block_rows // groups
    inverse, forward = tables(harmonics, samples)
    kinds = lax.dynamic_slice_in_dim(device_type, place * own_rows, own_rows, 0).reshape(-1)
    params = jnp.zeros((3, kinds.shape[0]), jnp.float32)
    for member in range(TYPES):
        params = (
            params
            + (kinds == member).astype(jnp.float32)[None, :] * device_table[:, member][:, None]
        )
    linear, amplitude, slope = (params[0], params[1], params[2])

    def time_of(spectrum):
        return jnp.dot(
            inverse,
            spectrum.reshape(2 * harmonics, -1),
            precision=top,
            preferred_element_type=jnp.float32,
        )

    def spectrum_of(signal):
        return jnp.dot(forward, signal, precision=top, preferred_element_type=jnp.float32).reshape(
            2, harmonics, own_rows, columns
        )

    def currents(spectrum):
        voltage = time_of(spectrum)
        bent = jnp.tanh(slope * voltage)
        flow = linear * voltage + amplitude * bent
        slopes_now = linear + amplitude * slope * (1.0 - bent * bent)
        return (spectrum_of(flow), slopes_now)

    field_state, field_source = (state, source)
    waves = place * local_harm + jnp.arange(local_harm, dtype=jnp.int32)

    def sides(field):
        padded = extended(field, (("node", 2),), 1)
        return (padded[:, :, :-2], padded[:, :, 2:])

    def across(field, local):
        moved = lax.all_to_all(field, "harm", split_axis=2, concat_axis=1, tiled=True)
        result, extra = local(moved)
        return (lax.all_to_all(result, "harm", split_axis=1, concat_axis=2, tiled=True), extra)

    def operator(field):
        above, below = sides(field)
        return stencil(field, above, below, capacity, row_shift, waves)

    spec_flow, slopes = across(field_state, currents)
    resid = operator(field_state) + spec_flow - field_source

    def linear_part(spectrum):
        return (spectrum_of(slopes * time_of(spectrum)), slopes)

    start = -resid
    beta = jnp.sqrt(lax.psum(jnp.sum(start * start), ("harm", "node")))
    basis = [start / beta]
    directions = []
    columns_h = []
    for iteration in range(ITERS):
        direction = precondition(basis[iteration], precond)
        directions.append(direction)
        coupled, unused = across(direction, linear_part)
        image = operator(direction) + coupled
        locals_dot = jnp.stack([jnp.sum(basis[member] * image) for member in range(iteration + 1)])
        totals, square = lax.psum((locals_dot, jnp.sum(image * image)), ("harm", "node"))
        heights = [totals[member] for member in range(iteration + 1)]
        for earlier in range(iteration + 1):
            image = image - heights[earlier] * basis[earlier]
        length = jnp.sqrt(square - jnp.sum(totals * totals))
        columns_h.append(
            jnp.stack(heights + [length] + [jnp.zeros((), jnp.float32)] * (ITERS - 1 - iteration))
        )
        if iteration + 1 < ITERS:
            basis.append(image / length)
    hess = jnp.stack(columns_h, axis=1)
    gram = jnp.dot(hess.T, hess, precision=top)
    coeffs = small_solve(gram, beta * hess[0])
    update = jnp.zeros_like(field_state)
    for iteration in range(ITERS):
        update = update + coeffs[iteration] * directions[iteration]
    return (update, resid)


ROUNDS = ITERS + 1
COLUMN_SHIFT = 1.0
MESH = pl.DeviceIdType.MESH


def split(value):
    high = value.astype(jnp.bfloat16)
    low = (value - high.astype(jnp.float32)).astype(jnp.bfloat16)
    return high, low


def wave_tables(groups, local_harm):
    harmonics = groups * local_harm
    samples = 2 * harmonics
    waves = np.arange(harmonics).reshape(groups, 1, local_harm)
    moments = np.arange(samples)[:, None, None, None]
    phase = (moments * waves[None] % samples) * (2.0 * np.pi / samples)
    inverse = np.concatenate([np.cos(phase), -np.sin(phase)], axis=2).reshape(samples, -1)
    weights = np.where(waves == 0, 1.0, 2.0) / samples
    weights = np.concatenate([weights, weights], axis=1).reshape(-1)
    forward = (inverse * weights[None]).T
    result = []
    for table in (inverse, forward):
        table = table.astype(np.float32)
        high = table.astype(jnp.bfloat16)
        low = (table - high.astype(np.float32)).astype(jnp.bfloat16)
        result.append(np.concatenate([high, low], axis=0))
    return np.stack(result)


def kernel(
    groups, blocks_count, dims,
    state, capacity, shifts, kinds, table, source_hbm, precond_hbm, waves_hbm,
    update_out, resid_out,
    fields, basis, arrived, answer, returned, image, slopes,
    source, precond, wave_mats, mat_high, mat_low, gram_send, gram_all,
    local_sems, out_send, out_recv, back_send, back_recv, halo_send, halo_recv, gram_ssem, gram_rsem,
):
    local_harm, rows, columns = dims
    own_rows = rows // groups
    pair = 2 * local_harm
    samples = 2 * groups * local_harm
    devices = groups * blocks_count
    place = lax.axis_index("harm")
    node = lax.axis_index("node")
    me = place * blocks_count + node

    loads = [
        pltpu.make_async_copy(precond_hbm, precond, local_sems.at[0]),
        pltpu.make_async_copy(waves_hbm, wave_mats, local_sems.at[1]),
        pltpu.make_async_copy(source_hbm, source, local_sems.at[2]),
    ]
    for load in loads:
        load.start()

    barrier = pltpu.get_barrier_semaphore()

    def greet(step, carry):
        other = lax.rem(me + step, devices)
        pl.semaphore_signal(
            barrier,
            inc=1,
            device_id=(other // blocks_count, lax.rem(other, blocks_count)),
            device_id_type=MESH,
        )
        return carry

    lax.fori_loop(1, devices, greet, 0)

    state_flat = state.reshape(2 * local_harm * rows, columns)
    for row in range(rows):
        for part in range(2):
            fields[0, 1 + row, part * local_harm:(part + 1) * local_harm, :] = state_flat[
                pl.ds(part * local_harm * rows + row, local_harm, stride=rows), :
            ]

    @pl.when(node == 0)
    def _():
        for q in range(ROUNDS):
            fields[q, 0] = jnp.zeros((pair, columns), jnp.float32)

    @pl.when(node == blocks_count - 1)
    def _():
        for q in range(ROUNDS):
            fields[q, rows + 1] = jnp.zeros((pair, columns), jnp.float32)

    pl.semaphore_wait(barrier, devices - 1)

    def out_copy(q, step):
        dest = lax.rem(place + step, groups)
        return pltpu.make_async_remote_copy(
            src_ref=fields.at[q, pl.ds(1 + dest * own_rows, own_rows)],
            dst_ref=arrived.at[q, :, place],
            send_sem=out_send.at[q, step],
            recv_sem=out_recv.at[q, step],
            device_id=(dest, node),
            device_id_type=MESH,
        )

    def back_copy(q, step):
        dest = lax.rem(place + step, groups)
        return pltpu.make_async_remote_copy(
            src_ref=answer.at[q, :, dest],
            dst_ref=returned.at[q, pl.ds(place * own_rows, own_rows)],
            send_sem=back_send.at[q, step],
            recv_sem=back_recv.at[q, step],
            device_id=(dest, node),
            device_id_type=MESH,
        )

    def halo_copy(q, up):
        return pltpu.make_async_remote_copy(
            src_ref=fields.at[q, 1 if up else rows],
            dst_ref=fields.at[q, rows + 1 if up else 0],
            send_sem=halo_send.at[q, up],
            recv_sem=halo_recv.at[q, up],
            device_id=(place, node - 1 if up else node + 1),
            device_id_type=MESH,
        )

    def each(copy, q, action):
        def step_of(step, carry):
            getattr(copy(q, step), action)()
            return carry

        lax.fori_loop(1, groups, step_of, 0)

    def halo(q, action):
        @pl.when(node > 0)
        def _():
            if action == "start":
                halo_copy(q, 1).start()
            else:
                halo_copy(q, 1).wait_send()
                halo_copy(q, 0).wait_recv()

        @pl.when(node < blocks_count - 1)
        def _():
            if action == "start":
                halo_copy(q, 0).start()
            else:
                halo_copy(q, 0).wait_send()
                halo_copy(q, 1).wait_recv()

    def send_out(q):
        each(out_copy, q, "start")
        halo(q, "start")
        arrived[q, :, place] = fields[q, pl.ds(1 + place * own_rows, own_rows)]

    def send_back(q, result):
        for row in range(own_rows):
            answer[q, row] = result[:, row * columns:(row + 1) * columns].reshape(
                groups, pair, columns
            )
        each(back_copy, q, "start")
        returned[q, pl.ds(place * own_rows, own_rows)] = answer[q, :, place]

    def transform(which, value):
        high, low = split(value)
        size = samples
        both = jnp.dot(wave_mats[which], high, preferred_element_type=jnp.float32)
        rest = jnp.dot(wave_mats[which, :size], low, preferred_element_type=jnp.float32)
        return both[:size] + (both[size:] + rest)

    def time_of(q):
        each(out_copy, q, "wait")
        lanes = [arrived[q, row].reshape(samples, columns) for row in range(own_rows)]
        return transform(0, jnp.concatenate(lanes, axis=1))

    harmonic = (place * local_harm + lax.broadcasted_iota(jnp.int32, (local_harm, columns), 0))
    rate = 0.05 * harmonic.astype(jnp.float32)

    def stencil(q):
        halo(q, "wait")

        def row_of(row, carry):
            here = fields[q, 1 + row]
            above = fields[q, row]
            below = fields[q, 2 + row]
            value = 4.0 * here - pltpu.roll(here, 1, 1) - pltpu.roll(here, columns - 1, 1) - below
            amount_here = shifts[row]
            for amount in range(SHIFTS):
                picked = jnp.where(amount_here == amount, 1.0, 0.0)
                moved = above if amount == 0 else pltpu.roll(above, columns - amount, 1)
                value = value - picked * moved
            reactive = rate * capacity[pl.ds(row, 1), :]
            turned = jnp.concatenate(
                [-reactive * here[local_harm:], reactive * here[:local_harm]], axis=0
            )
            image[row] = value + turned
            return carry

        lax.fori_loop(0, rows, row_of, 0, unroll=4)

    def precondition(q):
        given = basis.at[q].reshape(rows * pair, columns)
        taken = fields.at[q + 1].reshape((rows + 2) * pair, columns)
        for k in range(local_harm):
            real = given[pl.ds(k, rows, stride=pair), :]
            imag = given[pl.ds(local_harm + k, rows, stride=pair), :]
            high, low = split(jnp.concatenate([real, imag], axis=1))
            both = jnp.dot(
                jnp.concatenate([high, low], axis=0), mat_high[k], preferred_element_type=jnp.float32
            )
            rest = jnp.dot(high, mat_low[k], preferred_element_type=jnp.float32)
            value = both[:rows] + (both[rows:] + rest)
            taken[pl.ds(pair + k, rows, stride=pair), :] = value[:, :columns]
            taken[pl.ds(pair + local_harm + k, rows, stride=pair), :] = value[:, columns:]

    def inner(first, second):
        total = jnp.zeros((pair, columns), jnp.float32)
        for row in range(rows):
            total = total + basis[first, row] * basis[second, row]
        return jnp.sum(jnp.sum(total, axis=0, keepdims=True), axis=1, keepdims=True)

    send_out(0)

    loads[0].wait()

    def prepare(k, carry):
        real = precond[0, k].T
        imag = precond[1, k].T
        for part, left, right in ((0, real, imag), (1, -imag, real)):
            high, low = split(jnp.concatenate([left, right], axis=1))
            mat_high[k, part * columns:(part + 1) * columns, :] = high
            mat_low[k, part * columns:(part + 1) * columns, :] = low
        return carry

    lax.fori_loop(0, local_harm, prepare, 0)
    loads[1].wait()
    loads[2].wait()

    kind_rows = [kinds[pl.ds(place * own_rows + row, 1), :] for row in range(own_rows)]
    kind = jnp.concatenate(kind_rows, axis=1)
    params = []
    for member in range(3):
        value = jnp.zeros(kind.shape, jnp.float32)
        for which in range(TYPES):
            value = value + jnp.where(kind == which, 1.0, 0.0) * table[member, which]
        params.append(value)
    linear, amplitude, slope = params

    stencil(0)
    voltage = time_of(0)
    bent = jnp.tanh(slope * voltage)
    send_back(0, transform(1, linear * voltage + amplitude * bent))
    slopes[...] = linear + amplitude * slope * (1.0 - bent * bent)
    source_flat = source.reshape(2 * local_harm * rows, columns)
    for row in range(rows):
        for part in range(2):
            image[row, part * local_harm:(part + 1) * local_harm, :] -= source_flat[
                pl.ds(part * local_harm * rows + row, local_harm, stride=rows), :
            ]
    each(back_copy, 0, "wait")
    basis[0] = -(image[...] + returned[0])

    grams = {}
    for q in range(ITERS):
        precondition(q)
        send_out(q + 1)
        if q == 0:
            resid_out[...] = -basis[0]
        for other in range(q + 1):
            grams[other, q] = inner(other, q)
        stencil(q + 1)
        image[...] = image[...] - COLUMN_SHIFT * basis[q]
        send_back(q + 1, transform(1, slopes[...] * time_of(q + 1)))
        each(back_copy, q + 1, "wait")
        basis[q + 1] = image[...] + returned[q + 1]
    for other in range(ITERS + 1):
        grams[other, ITERS] = inner(other, ITERS)

    lane = lax.broadcasted_iota(jnp.int32, (1, 128), 1)
    packed = jnp.zeros((1, 128), jnp.float32)
    names = sorted(grams)
    for at, name in enumerate(names):
        packed = packed + jnp.where(lane == at, grams[name], 0.0)
    gram_send[...] = packed
    gram_all[me] = packed

    def gram_copy(step):
        other = lax.rem(me + step, devices)
        return pltpu.make_async_remote_copy(
            src_ref=gram_send,
            dst_ref=gram_all.at[me],
            send_sem=gram_ssem.at[step],
            recv_sem=gram_rsem.at[step],
            device_id=(other // blocks_count, lax.rem(other, blocks_count)),
            device_id_type=MESH,
        )

    def gram_start(step, carry):
        gram_copy(step).start()
        return carry

    def gram_wait(step, carry):
        gram_copy(step).wait()
        return carry

    lax.fori_loop(1, devices, gram_start, 0)
    lax.fori_loop(1, devices, gram_wait, 0)
    total = jnp.sum(gram_all[...], axis=0)
    full = {}
    for at, name in enumerate(names):
        value = jnp.sum(jnp.where(lane == at, total, 0.0), axis=1, keepdims=True)
        full[name] = full[name[::-1]] = value
    half = {}
    for a in range(ITERS + 1):
        for j in range(ITERS):
            half[a, j] = full[a, j + 1] + COLUMN_SHIFT * full[a, j]
    normal = {}
    for i in range(ITERS):
        for j in range(ITERS):
            normal[i, j] = half[i + 1, j] + COLUMN_SHIFT * half[i, j]
    right = [half[0, j] for j in range(ITERS)]
    lower, diag = {}, []
    for j in range(ITERS):
        value = normal[j, j]
        for m in range(j):
            value = value - lower[j, m] * lower[j, m] * diag[m]
        diag.append(value)
        for i in range(j + 1, ITERS):
            value = normal[i, j]
            for m in range(j):
                value = value - lower[i, m] * lower[j, m] * diag[m]
            lower[i, j] = value / diag[j]
    forward = []
    for j in range(ITERS):
        value = right[j]
        for m in range(j):
            value = value - lower[j, m] * forward[m]
        forward.append(value)
    coeffs = [None] * ITERS
    for j in reversed(range(ITERS)):
        value = forward[j] / diag[j]
        for m in range(j + 1, ITERS):
            value = value - lower[m, j] * coeffs[m]
        coeffs[j] = value
    for row in range(rows):
        value = coeffs[0] * fields[1, 1 + row]
        for j in range(1, ITERS):
            value = value + coeffs[j] * fields[j + 1, 1 + row]
        update_out[row] = value


def fused(state, source, capacity, row_shift, device_type, device_table, precond):
    groups = lax.axis_size("harm")
    blocks_count = lax.axis_size("node")
    _, local_harm, rows, columns = state.shape
    own_rows = rows // groups
    pair = 2 * local_harm
    samples = 2 * groups * local_harm
    devices = groups * blocks_count
    waves = jnp.asarray(wave_tables(groups, local_harm))
    vmem = pl.BlockSpec(memory_space=pltpu.VMEM)
    smem = pl.BlockSpec(memory_space=pltpu.SMEM)
    anywhere = pl.BlockSpec(memory_space=pl.ANY)
    field = (rows, pair, columns)
    f32 = jnp.float32
    dma = pltpu.SemaphoreType.DMA
    update, resid = pl.pallas_call(
        functools.partial(kernel, groups, blocks_count, (local_harm, rows, columns)),
        out_shape=(jax.ShapeDtypeStruct(field, f32),) * 2,
        in_specs=[vmem, vmem, smem, vmem, smem, anywhere, anywhere, anywhere],
        out_specs=(vmem, vmem),
        scratch_shapes=[
            pltpu.VMEM((ROUNDS, rows + 2, pair, columns), f32),
            pltpu.VMEM((ROUNDS,) + field, f32),
            pltpu.VMEM((ROUNDS, own_rows, groups, pair, columns), f32),
            pltpu.VMEM((ROUNDS, own_rows, groups, pair, columns), f32),
            pltpu.VMEM((ROUNDS,) + field, f32),
            pltpu.VMEM(field, f32),
            pltpu.VMEM((samples, own_rows * columns), f32),
            pltpu.VMEM(source.shape, f32),
            pltpu.VMEM(precond.shape, f32),
            pltpu.VMEM(waves.shape, jnp.bfloat16),
            pltpu.VMEM((local_harm, 2 * columns, 2 * columns), jnp.bfloat16),
            pltpu.VMEM((local_harm, 2 * columns, 2 * columns), jnp.bfloat16),
            pltpu.VMEM((1, 128), f32),
            pltpu.VMEM((devices, 1, 128), f32),
            dma((3,)),
            dma((ROUNDS, groups)),
            dma((ROUNDS, groups)),
            dma((ROUNDS, groups)),
            dma((ROUNDS, groups)),
            dma((ROUNDS, 2)),
            dma((ROUNDS, 2)),
            dma((devices,)),
            dma((devices,)),
        ],
        compiler_params=pltpu.CompilerParams(
            collective_id=0, has_side_effects=True, vmem_limit_bytes=40 * 1024 * 1024
        ),
    )(state, capacity, row_shift, device_type, device_table, source, precond, waves)
    return back(update, state.shape), back(resid, state.shape)


def back(value, shape):
    parts, local_harm, rows, columns = shape
    return jnp.transpose(value.reshape(rows, parts, local_harm, columns), (1, 2, 0, 3))


def chosen(*args):
    groups = lax.axis_size("harm")
    _, local_harm, rows, columns = args[0].shape
    if local_harm % 16 or rows % 16 or rows % groups or columns % 128:
        return body(*args)
    return fused(*args)


def solution(mesh):
    return jax.shard_map(
        chosen,
        mesh=mesh,
        in_specs=(
            P(None, "harm", "node", None),
            P(None, "harm", "node", None),
            P("node", None),
            P("node"),
            P("node", None),
            P(),
            P(None, "harm", None, None),
        ),
        out_specs=(P(None, "harm", "node", None), P(None, "harm", "node", None)),
        check_vma=False,
    )
```

```python
import functools

import jax
import jax.numpy as jnp
import numpy as np
from jax import lax
from jax.experimental import pallas as pl
from jax.experimental.pallas import tpu as pltpu
from jax.sharding import PartitionSpec as P

ITERS = 3
TYPES = 4
SHIFTS = 4


omega_step = 0.05
top = lax.Precision.HIGHEST


def extended(cells, sides, width):
    for axis, dim in sides:
        count = lax.axis_size(axis)
        ends = count - 1
        head = lax.slice_in_dim(cells, 0, width, axis=dim)
        tail = lax.slice_in_dim(cells, cells.shape[dim] - width, cells.shape[dim], axis=dim)
        cells = jnp.concatenate(
            [
                lax.ppermute(tail, axis, [(i, (i + 1) % count) for i in range(ends)]),
                cells,
                lax.ppermute(head, axis, [((i + 1) % count, i) for i in range(ends)]),
            ],
            axis=dim,
        )
    return cells


def small_solve(gram, right):
    lower = jnp.linalg.cholesky(gram)
    order = gram.shape[0]
    forward = []
    for column in range(order):
        value = right[column]
        for member in range(column):
            value = value - lower[column, member] * forward[member]
        forward.append(value / lower[column, column])
    result = [None] * order
    for column in reversed(range(order)):
        value = forward[column]
        for member in range(column + 1, order):
            value = value - lower[member, column] * result[member]
        result[column] = value / lower[column, column]
    return result


def tables(harmonics, samples):
    waves = jnp.arange(harmonics, dtype=jnp.int32)
    moments = jnp.arange(samples, dtype=jnp.int32)
    phase = (moments[:, None] * waves[None, :] % samples).astype(jnp.float32) * (
        2.0 * jnp.pi / samples
    )
    cosine = jnp.cos(phase)
    sine = jnp.sin(phase)
    inverse = jnp.concatenate([cosine, -sine], axis=1)
    weights = jnp.where(waves == 0, 1.0, 2.0).astype(jnp.float32) / samples
    forward = jnp.concatenate([cosine.T * weights[:, None], -sine.T * weights[:, None]], axis=0)
    return (inverse, forward)


def stencil(field, above, below, capacity, shifts, waves):
    left_side = jnp.roll(field, 1, axis=3)
    right_side = jnp.roll(field, -1, axis=3)
    skewed = jnp.zeros_like(field)
    for amount in range(SHIFTS):
        picked = (shifts == amount).astype(jnp.float32)[None, None, :, None]
        skewed = skewed + picked * jnp.roll(above, -amount, axis=3)
    result = 4.0 * field - left_side - right_side - skewed - below
    reactive = omega_step * waves.astype(jnp.float32)[:, None, None] * capacity[None]
    return result + jnp.stack([-reactive * field[1], reactive * field[0]])


def precondition(field, blocks):
    real_part = jnp.einsum("krd,kcd->krc", field[0], blocks[0], precision=top) - jnp.einsum(
        "krd,kcd->krc", field[1], blocks[1], precision=top
    )
    imag_part = jnp.einsum("krd,kcd->krc", field[0], blocks[1], precision=top) + jnp.einsum(
        "krd,kcd->krc", field[1], blocks[0], precision=top
    )
    return jnp.stack([real_part, imag_part])


def body(state, source, capacity, row_shift, device_type, device_table, precond):
    groups = lax.axis_size("harm")
    place = lax.axis_index("harm")
    local_harm = state.shape[1]
    block_rows = state.shape[2]
    columns = state.shape[3]
    harmonics = local_harm * groups
    samples = 2 * harmonics
    own_rows = block_rows // groups
    inverse, forward = tables(harmonics, samples)
    kinds = lax.dynamic_slice_in_dim(device_type, place * own_rows, own_rows, 0).reshape(-1)
    params = jnp.zeros((3, kinds.shape[0]), jnp.float32)
    for member in range(TYPES):
        params = (
            params
            + (kinds == member).astype(jnp.float32)[None, :] * device_table[:, member][:, None]
        )
    linear, amplitude, slope = (params[0], params[1], params[2])

    def time_of(spectrum):
        return jnp.dot(
            inverse,
            spectrum.reshape(2 * harmonics, -1),
            precision=top,
            preferred_element_type=jnp.float32,
        )

    def spectrum_of(signal):
        return jnp.dot(forward, signal, precision=top, preferred_element_type=jnp.float32).reshape(
            2, harmonics, own_rows, columns
        )

    def currents(spectrum):
        voltage = time_of(spectrum)
        bent = jnp.tanh(slope * voltage)
        flow = linear * voltage + amplitude * bent
        slopes_now = linear + amplitude * slope * (1.0 - bent * bent)
        return (spectrum_of(flow), slopes_now)

    field_state, field_source = (state, source)
    waves = place * local_harm + jnp.arange(local_harm, dtype=jnp.int32)

    def sides(field):
        padded = extended(field, (("node", 2),), 1)
        return (padded[:, :, :-2], padded[:, :, 2:])

    def across(field, local):
        moved = lax.all_to_all(field, "harm", split_axis=2, concat_axis=1, tiled=True)
        result, extra = local(moved)
        return (lax.all_to_all(result, "harm", split_axis=1, concat_axis=2, tiled=True), extra)

    def operator(field):
        above, below = sides(field)
        return stencil(field, above, below, capacity, row_shift, waves)

    spec_flow, slopes = across(field_state, currents)
    resid = operator(field_state) + spec_flow - field_source

    def linear_part(spectrum):
        return (spectrum_of(slopes * time_of(spectrum)), slopes)

    start = -resid
    beta = jnp.sqrt(lax.psum(jnp.sum(start * start), ("harm", "node")))
    basis = [start / beta]
    directions = []
    columns_h = []
    for iteration in range(ITERS):
        direction = precondition(basis[iteration], precond)
        directions.append(direction)
        coupled, unused = across(direction, linear_part)
        image = operator(direction) + coupled
        locals_dot = jnp.stack([jnp.sum(basis[member] * image) for member in range(iteration + 1)])
        totals, square = lax.psum((locals_dot, jnp.sum(image * image)), ("harm", "node"))
        heights = [totals[member] for member in range(iteration + 1)]
        for earlier in range(iteration + 1):
            image = image - heights[earlier] * basis[earlier]
        length = jnp.sqrt(square - jnp.sum(totals * totals))
        columns_h.append(
            jnp.stack(heights + [length] + [jnp.zeros((), jnp.float32)] * (ITERS - 1 - iteration))
        )
        if iteration + 1 < ITERS:
            basis.append(image / length)
    hess = jnp.stack(columns_h, axis=1)
    gram = jnp.dot(hess.T, hess, precision=top)
    coeffs = small_solve(gram, beta * hess[0])
    update = jnp.zeros_like(field_state)
    for iteration in range(ITERS):
        update = update + coeffs[iteration] * directions[iteration]
    return (update, resid)


ROUNDS = ITERS + 1
COLUMN_SHIFT = 1.0
MESH = pl.DeviceIdType.MESH


def split(value):
    high = value.astype(jnp.bfloat16)
    low = (value - high.astype(jnp.float32)).astype(jnp.bfloat16)
    return high, low


def wave_tables(groups, local_harm):
    harmonics = groups * local_harm
    samples = 2 * harmonics
    waves = np.arange(harmonics).reshape(groups, 1, local_harm)
    moments = np.arange(samples)[:, None, None, None]
    phase = (moments * waves[None] % samples) * (2.0 * np.pi / samples)
    inverse = np.concatenate([np.cos(phase), -np.sin(phase)], axis=2).reshape(samples, -1)
    weights = np.where(waves == 0, 1.0, 2.0) / samples
    weights = np.concatenate([weights, weights], axis=1).reshape(-1)
    forward = (inverse * weights[None]).T
    result = []
    for table in (inverse, forward):
        table = table.astype(np.float32)
        high = table.astype(jnp.bfloat16)
        low = (table - high.astype(np.float32)).astype(jnp.bfloat16)
        result.append(np.concatenate([high, low], axis=0))
    return np.stack(result)


def kernel(
    groups, blocks_count, dims,
    state_hbm, capacity_hbm, shifts_hbm, kinds_hbm, table_hbm, source_hbm, precond_hbm, waves_hbm,
    update_out, resid_out,
    fields, basis, arrived, answer, returned, image, slopes,
    state, capacity, shifts, kinds, table, source, precond, wave_mats, mat_high, mat_low, gram_send, gram_all,
    local_sems, out_send, out_recv, back_send, back_recv, halo_send, halo_recv, gram_ssem, gram_rsem,
):
    local_harm, rows, columns = dims
    own_rows = rows // groups
    pair = 2 * local_harm
    samples = 2 * groups * local_harm
    devices = groups * blocks_count
    place = lax.axis_index("harm")
    node = lax.axis_index("node")
    me = place * blocks_count + node

    loads = [
        pltpu.make_async_copy(precond_hbm, precond, local_sems.at[0]),
        pltpu.make_async_copy(waves_hbm, wave_mats, local_sems.at[1]),
        pltpu.make_async_copy(source_hbm, source, local_sems.at[2]),
        pltpu.make_async_copy(capacity_hbm, capacity, local_sems.at[3]),
        pltpu.make_async_copy(shifts_hbm, shifts, local_sems.at[4]),
        pltpu.make_async_copy(kinds_hbm, kinds, local_sems.at[5]),
        pltpu.make_async_copy(table_hbm, table, local_sems.at[6]),
    ]
    first_load = pltpu.make_async_copy(state_hbm, state, local_sems.at[7])
    first_load.start()
    for load in loads:
        load.start()

    barrier = pltpu.get_barrier_semaphore()

    def greet(step, carry):
        other = lax.rem(me + step, devices)
        pl.semaphore_signal(
            barrier,
            inc=1,
            device_id=(other // blocks_count, lax.rem(other, blocks_count)),
            device_id_type=MESH,
        )
        return carry

    lax.fori_loop(1, devices, greet, 0)

    first_load.wait()
    state_flat = state.reshape(2 * local_harm * rows, columns)
    for row in range(rows):
        for part in range(2):
            fields[0, 1 + row, part * local_harm:(part + 1) * local_harm, :] = state_flat[
                pl.ds(part * local_harm * rows + row, local_harm, stride=rows), :
            ]

    @pl.when(node == 0)
    def _():
        for q in range(ROUNDS):
            fields[q, 0] = jnp.zeros((pair, columns), jnp.float32)

    @pl.when(node == blocks_count - 1)
    def _():
        for q in range(ROUNDS):
            fields[q, rows + 1] = jnp.zeros((pair, columns), jnp.float32)

    pl.semaphore_wait(barrier, devices - 1)

    def out_copy(q, step):
        dest = lax.rem(place + step, groups)
        return pltpu.make_async_remote_copy(
            src_ref=fields.at[q, pl.ds(1 + dest * own_rows, own_rows)],
            dst_ref=arrived.at[q, :, place],
            send_sem=out_send.at[q, step],
            recv_sem=out_recv.at[q, step],
            device_id=(dest, node),
            device_id_type=MESH,
        )

    def back_copy(q, step):
        dest = lax.rem(place + step, groups)
        return pltpu.make_async_remote_copy(
            src_ref=answer.at[q, :, dest],
            dst_ref=returned.at[q, pl.ds(place * own_rows, own_rows)],
            send_sem=back_send.at[q, step],
            recv_sem=back_recv.at[q, step],
            device_id=(dest, node),
            device_id_type=MESH,
        )

    def halo_copy(q, up):
        return pltpu.make_async_remote_copy(
            src_ref=fields.at[q, 1 if up else rows],
            dst_ref=fields.at[q, rows + 1 if up else 0],
            send_sem=halo_send.at[q, up],
            recv_sem=halo_recv.at[q, up],
            device_id=(place, node - 1 if up else node + 1),
            device_id_type=MESH,
        )

    def each(copy, q, action):
        def step_of(step, carry):
            getattr(copy(q, step), action)()
            return carry

        lax.fori_loop(1, groups, step_of, 0)

    def halo(q, action):
        @pl.when(node > 0)
        def _():
            if action == "start":
                halo_copy(q, 1).start()
            else:
                halo_copy(q, 1).wait_send()
                halo_copy(q, 0).wait_recv()

        @pl.when(node < blocks_count - 1)
        def _():
            if action == "start":
                halo_copy(q, 0).start()
            else:
                halo_copy(q, 0).wait_send()
                halo_copy(q, 1).wait_recv()

    def send_out(q):
        each(out_copy, q, "start")
        halo(q, "start")
        arrived[q, :, place] = fields[q, pl.ds(1 + place * own_rows, own_rows)]

    def send_back(q, result):
        for row in range(own_rows):
            answer[q, row] = result[:, row * columns:(row + 1) * columns].reshape(
                groups, pair, columns
            )
        each(back_copy, q, "start")
        returned[q, pl.ds(place * own_rows, own_rows)] = answer[q, :, place]

    def transform(which, value):
        high, low = split(value)
        size = samples
        both = jnp.dot(wave_mats[which], high, preferred_element_type=jnp.float32)
        rest = jnp.dot(wave_mats[which, :size], low, preferred_element_type=jnp.float32)
        return both[:size] + (both[size:] + rest)

    def time_of(q):
        each(out_copy, q, "wait")
        lanes = [arrived[q, row].reshape(samples, columns) for row in range(own_rows)]
        return transform(0, jnp.concatenate(lanes, axis=1))

    harmonic = (place * local_harm + lax.broadcasted_iota(jnp.int32, (local_harm, columns), 0))
    rate = 0.05 * harmonic.astype(jnp.float32)

    def stencil(q):
        halo(q, "wait")

        def row_of(row, carry):
            here = fields[q, 1 + row]
            above = fields[q, row]
            below = fields[q, 2 + row]
            value = 4.0 * here - pltpu.roll(here, 1, 1) - pltpu.roll(here, columns - 1, 1) - below
            amount_here = shifts[row]
            for amount in range(SHIFTS):
                picked = jnp.where(amount_here == amount, 1.0, 0.0)
                moved = above if amount == 0 else pltpu.roll(above, columns - amount, 1)
                value = value - picked * moved
            reactive = rate * capacity[pl.ds(row, 1), :]
            turned = jnp.concatenate(
                [-reactive * here[local_harm:], reactive * here[:local_harm]], axis=0
            )
            image[row] = value + turned
            return carry

        lax.fori_loop(0, rows, row_of, 0, unroll=4)

    def precondition(q):
        given = basis.at[q].reshape(rows * pair, columns)
        taken = fields.at[q + 1].reshape((rows + 2) * pair, columns)
        for k in range(local_harm):
            real = given[pl.ds(k, rows, stride=pair), :]
            imag = given[pl.ds(local_harm + k, rows, stride=pair), :]
            high, low = split(jnp.concatenate([real, imag], axis=1))
            both = jnp.dot(
                jnp.concatenate([high, low], axis=0), mat_high[k], preferred_element_type=jnp.float32
            )
            rest = jnp.dot(high, mat_low[k], preferred_element_type=jnp.float32)
            value = both[:rows] + (both[rows:] + rest)
            taken[pl.ds(pair + k, rows, stride=pair), :] = value[:, :columns]
            taken[pl.ds(pair + local_harm + k, rows, stride=pair), :] = value[:, columns:]

    def inner(first, second):
        total = jnp.zeros((pair, columns), jnp.float32)
        for row in range(rows):
            total = total + basis[first, row] * basis[second, row]
        return jnp.sum(jnp.sum(total, axis=0, keepdims=True), axis=1, keepdims=True)

    send_out(0)

    loads[0].wait()

    def prepare(k, carry):
        real = precond[0, k].T
        imag = precond[1, k].T
        for part, left, right in ((0, real, imag), (1, -imag, real)):
            high, low = split(jnp.concatenate([left, right], axis=1))
            mat_high[k, part * columns:(part + 1) * columns, :] = high
            mat_low[k, part * columns:(part + 1) * columns, :] = low
        return carry

    lax.fori_loop(0, local_harm, prepare, 0)
    for load in loads[1:]:
        load.wait()

    kind_rows = [kinds[pl.ds(place * own_rows + row, 1), :] for row in range(own_rows)]
    kind = jnp.concatenate(kind_rows, axis=1)
    params = []
    for member in range(3):
        value = jnp.zeros(kind.shape, jnp.float32)
        for which in range(TYPES):
            value = value + jnp.where(kind == which, 1.0, 0.0) * table[member, which]
        params.append(value)
    linear, amplitude, slope = params

    stencil(0)
    voltage = time_of(0)
    bent = jnp.tanh(slope * voltage)
    send_back(0, transform(1, linear * voltage + amplitude * bent))
    slopes[...] = linear + amplitude * slope * (1.0 - bent * bent)
    source_flat = source.reshape(2 * local_harm * rows, columns)
    for row in range(rows):
        for part in range(2):
            image[row, part * local_harm:(part + 1) * local_harm, :] -= source_flat[
                pl.ds(part * local_harm * rows + row, local_harm, stride=rows), :
            ]
    each(back_copy, 0, "wait")
    basis[0] = -(image[...] + returned[0])

    grams = {}
    for q in range(ITERS):
        precondition(q)
        send_out(q + 1)
        if q == 0:
            resid_out[...] = -basis[0]
        for other in range(q + 1):
            grams[other, q] = inner(other, q)
        stencil(q + 1)
        image[...] = image[...] - COLUMN_SHIFT * basis[q]
        send_back(q + 1, transform(1, slopes[...] * time_of(q + 1)))
        each(back_copy, q + 1, "wait")
        basis[q + 1] = image[...] + returned[q + 1]
    for other in range(ITERS + 1):
        grams[other, ITERS] = inner(other, ITERS)

    lane = lax.broadcasted_iota(jnp.int32, (1, 128), 1)
    packed = jnp.zeros((1, 128), jnp.float32)
    names = sorted(grams)
    for at, name in enumerate(names):
        packed = packed + jnp.where(lane == at, grams[name], 0.0)
    gram_send[...] = packed
    gram_all[me] = packed

    def gram_copy(step):
        other = lax.rem(me + step, devices)
        return pltpu.make_async_remote_copy(
            src_ref=gram_send,
            dst_ref=gram_all.at[me],
            send_sem=gram_ssem.at[step],
            recv_sem=gram_rsem.at[step],
            device_id=(other // blocks_count, lax.rem(other, blocks_count)),
            device_id_type=MESH,
        )

    def gram_start(step, carry):
        gram_copy(step).start()
        return carry

    def gram_wait(step, carry):
        gram_copy(step).wait()
        return carry

    lax.fori_loop(1, devices, gram_start, 0)
    lax.fori_loop(1, devices, gram_wait, 0)
    total = jnp.sum(gram_all[...], axis=0)
    full = {}
    for at, name in enumerate(names):
        value = jnp.sum(jnp.where(lane == at, total, 0.0), axis=1, keepdims=True)
        full[name] = full[name[::-1]] = value
    half = {}
    for a in range(ITERS + 1):
        for j in range(ITERS):
            half[a, j] = full[a, j + 1] + COLUMN_SHIFT * full[a, j]
    normal = {}
    for i in range(ITERS):
        for j in range(ITERS):
            normal[i, j] = half[i + 1, j] + COLUMN_SHIFT * half[i, j]
    right = [half[0, j] for j in range(ITERS)]
    lower, diag = {}, []
    for j in range(ITERS):
        value = normal[j, j]
        for m in range(j):
            value = value - lower[j, m] * lower[j, m] * diag[m]
        diag.append(value)
        for i in range(j + 1, ITERS):
            value = normal[i, j]
            for m in range(j):
                value = value - lower[i, m] * lower[j, m] * diag[m]
            lower[i, j] = value / diag[j]
    forward = []
    for j in range(ITERS):
        value = right[j]
        for m in range(j):
            value = value - lower[j, m] * forward[m]
        forward.append(value)
    coeffs = [None] * ITERS
    for j in reversed(range(ITERS)):
        value = forward[j] / diag[j]
        for m in range(j + 1, ITERS):
            value = value - lower[m, j] * coeffs[m]
        coeffs[j] = value
    for row in range(rows):
        value = coeffs[0] * fields[1, 1 + row]
        for j in range(1, ITERS):
            value = value + coeffs[j] * fields[j + 1, 1 + row]
        update_out[row] = value


def fused(state, source, capacity, row_shift, device_type, device_table, precond):
    groups = lax.axis_size("harm")
    blocks_count = lax.axis_size("node")
    _, local_harm, rows, columns = state.shape
    own_rows = rows // groups
    pair = 2 * local_harm
    samples = 2 * groups * local_harm
    devices = groups * blocks_count
    waves = jnp.asarray(wave_tables(groups, local_harm))
    vmem = pl.BlockSpec(memory_space=pltpu.VMEM)
    anywhere = pl.BlockSpec(memory_space=pl.ANY)
    field = (rows, pair, columns)
    f32 = jnp.float32
    dma = pltpu.SemaphoreType.DMA
    update, resid = pl.pallas_call(
        functools.partial(kernel, groups, blocks_count, (local_harm, rows, columns)),
        out_shape=(jax.ShapeDtypeStruct(field, f32),) * 2,
        in_specs=[anywhere] * 8,
        out_specs=(vmem, vmem),
        scratch_shapes=[
            pltpu.VMEM((ROUNDS, rows + 2, pair, columns), f32),
            pltpu.VMEM((ROUNDS,) + field, f32),
            pltpu.VMEM((ROUNDS, own_rows, groups, pair, columns), f32),
            pltpu.VMEM((ROUNDS, own_rows, groups, pair, columns), f32),
            pltpu.VMEM((ROUNDS,) + field, f32),
            pltpu.VMEM(field, f32),
            pltpu.VMEM((samples, own_rows * columns), f32),
            pltpu.VMEM(state.shape, f32),
            pltpu.VMEM(capacity.shape, f32),
            pltpu.SMEM(row_shift.shape, jnp.int32),
            pltpu.VMEM(device_type.shape, jnp.int32),
            pltpu.SMEM(device_table.shape, f32),
            pltpu.VMEM(source.shape, f32),
            pltpu.VMEM(precond.shape, f32),
            pltpu.VMEM(waves.shape, jnp.bfloat16),
            pltpu.VMEM((local_harm, 2 * columns, 2 * columns), jnp.bfloat16),
            pltpu.VMEM((local_harm, 2 * columns, 2 * columns), jnp.bfloat16),
            pltpu.VMEM((1, 128), f32),
            pltpu.VMEM((devices, 1, 128), f32),
            dma((8,)),
            dma((ROUNDS, groups)),
            dma((ROUNDS, groups)),
            dma((ROUNDS, groups)),
            dma((ROUNDS, groups)),
            dma((ROUNDS, 2)),
            dma((ROUNDS, 2)),
            dma((devices,)),
            dma((devices,)),
        ],
        compiler_params=pltpu.CompilerParams(
            collective_id=0, has_side_effects=True, vmem_limit_bytes=67043328
        ),
    )(state, capacity, row_shift, device_type, device_table, source, precond, waves)
    return back(update, state.shape), back(resid, state.shape)


def back(value, shape):
    parts, local_harm, rows, columns = shape
    return jnp.transpose(value.reshape(rows, parts, local_harm, columns), (1, 2, 0, 3))


def chosen(*args):
    groups = lax.axis_size("harm")
    _, local_harm, rows, columns = args[0].shape
    if local_harm % 16 or rows % 16 or rows % groups or columns % 128:
        return body(*args)
    return fused(*args)


def solution(mesh):
    return jax.shard_map(
        chosen,
        mesh=mesh,
        in_specs=(
            P(None, "harm", "node", None),
            P(None, "harm", "node", None),
            P("node", None),
            P("node"),
            P("node", None),
            P(),
            P(None, "harm", None, None),
        ),
        out_specs=(P(None, "harm", "node", None), P(None, "harm", "node", None)),
        check_vma=False,
    )
```

```python
import functools

import jax
import jax.numpy as jnp
import numpy as np
from jax import lax
from jax.experimental import pallas as pl
from jax.experimental.pallas import tpu as pltpu
from jax.sharding import PartitionSpec as P

ITERS = 3
TYPES = 4
SHIFTS = 4


omega_step = 0.05
top = lax.Precision.HIGHEST


def extended(cells, sides, width):
    for axis, dim in sides:
        count = lax.axis_size(axis)
        ends = count - 1
        head = lax.slice_in_dim(cells, 0, width, axis=dim)
        tail = lax.slice_in_dim(cells, cells.shape[dim] - width, cells.shape[dim], axis=dim)
        cells = jnp.concatenate(
            [
                lax.ppermute(tail, axis, [(i, (i + 1) % count) for i in range(ends)]),
                cells,
                lax.ppermute(head, axis, [((i + 1) % count, i) for i in range(ends)]),
            ],
            axis=dim,
        )
    return cells


def small_solve(gram, right):
    lower = jnp.linalg.cholesky(gram)
    order = gram.shape[0]
    forward = []
    for column in range(order):
        value = right[column]
        for member in range(column):
            value = value - lower[column, member] * forward[member]
        forward.append(value / lower[column, column])
    result = [None] * order
    for column in reversed(range(order)):
        value = forward[column]
        for member in range(column + 1, order):
            value = value - lower[member, column] * result[member]
        result[column] = value / lower[column, column]
    return result


def tables(harmonics, samples):
    waves = jnp.arange(harmonics, dtype=jnp.int32)
    moments = jnp.arange(samples, dtype=jnp.int32)
    phase = (moments[:, None] * waves[None, :] % samples).astype(jnp.float32) * (
        2.0 * jnp.pi / samples
    )
    cosine = jnp.cos(phase)
    sine = jnp.sin(phase)
    inverse = jnp.concatenate([cosine, -sine], axis=1)
    weights = jnp.where(waves == 0, 1.0, 2.0).astype(jnp.float32) / samples
    forward = jnp.concatenate([cosine.T * weights[:, None], -sine.T * weights[:, None]], axis=0)
    return (inverse, forward)


def stencil(field, above, below, capacity, shifts, waves):
    left_side = jnp.roll(field, 1, axis=3)
    right_side = jnp.roll(field, -1, axis=3)
    skewed = jnp.zeros_like(field)
    for amount in range(SHIFTS):
        picked = (shifts == amount).astype(jnp.float32)[None, None, :, None]
        skewed = skewed + picked * jnp.roll(above, -amount, axis=3)
    result = 4.0 * field - left_side - right_side - skewed - below
    reactive = omega_step * waves.astype(jnp.float32)[:, None, None] * capacity[None]
    return result + jnp.stack([-reactive * field[1], reactive * field[0]])


def precondition(field, blocks):
    real_part = jnp.einsum("krd,kcd->krc", field[0], blocks[0], precision=top) - jnp.einsum(
        "krd,kcd->krc", field[1], blocks[1], precision=top
    )
    imag_part = jnp.einsum("krd,kcd->krc", field[0], blocks[1], precision=top) + jnp.einsum(
        "krd,kcd->krc", field[1], blocks[0], precision=top
    )
    return jnp.stack([real_part, imag_part])


def body(state, source, capacity, row_shift, device_type, device_table, precond):
    groups = lax.axis_size("harm")
    place = lax.axis_index("harm")
    local_harm = state.shape[1]
    block_rows = state.shape[2]
    columns = state.shape[3]
    harmonics = local_harm * groups
    samples = 2 * harmonics
    own_rows = block_rows // groups
    inverse, forward = tables(harmonics, samples)
    kinds = lax.dynamic_slice_in_dim(device_type, place * own_rows, own_rows, 0).reshape(-1)
    params = jnp.zeros((3, kinds.shape[0]), jnp.float32)
    for member in range(TYPES):
        params = (
            params
            + (kinds == member).astype(jnp.float32)[None, :] * device_table[:, member][:, None]
        )
    linear, amplitude, slope = (params[0], params[1], params[2])

    def time_of(spectrum):
        return jnp.dot(
            inverse,
            spectrum.reshape(2 * harmonics, -1),
            precision=top,
            preferred_element_type=jnp.float32,
        )

    def spectrum_of(signal):
        return jnp.dot(forward, signal, precision=top, preferred_element_type=jnp.float32).reshape(
            2, harmonics, own_rows, columns
        )

    def currents(spectrum):
        voltage = time_of(spectrum)
        bent = jnp.tanh(slope * voltage)
        flow = linear * voltage + amplitude * bent
        slopes_now = linear + amplitude * slope * (1.0 - bent * bent)
        return (spectrum_of(flow), slopes_now)

    field_state, field_source = (state, source)
    waves = place * local_harm + jnp.arange(local_harm, dtype=jnp.int32)

    def sides(field):
        padded = extended(field, (("node", 2),), 1)
        return (padded[:, :, :-2], padded[:, :, 2:])

    def across(field, local):
        moved = lax.all_to_all(field, "harm", split_axis=2, concat_axis=1, tiled=True)
        result, extra = local(moved)
        return (lax.all_to_all(result, "harm", split_axis=1, concat_axis=2, tiled=True), extra)

    def operator(field):
        above, below = sides(field)
        return stencil(field, above, below, capacity, row_shift, waves)

    spec_flow, slopes = across(field_state, currents)
    resid = operator(field_state) + spec_flow - field_source

    def linear_part(spectrum):
        return (spectrum_of(slopes * time_of(spectrum)), slopes)

    start = -resid
    beta = jnp.sqrt(lax.psum(jnp.sum(start * start), ("harm", "node")))
    basis = [start / beta]
    directions = []
    columns_h = []
    for iteration in range(ITERS):
        direction = precondition(basis[iteration], precond)
        directions.append(direction)
        coupled, unused = across(direction, linear_part)
        image = operator(direction) + coupled
        locals_dot = jnp.stack([jnp.sum(basis[member] * image) for member in range(iteration + 1)])
        totals, square = lax.psum((locals_dot, jnp.sum(image * image)), ("harm", "node"))
        heights = [totals[member] for member in range(iteration + 1)]
        for earlier in range(iteration + 1):
            image = image - heights[earlier] * basis[earlier]
        length = jnp.sqrt(square - jnp.sum(totals * totals))
        columns_h.append(
            jnp.stack(heights + [length] + [jnp.zeros((), jnp.float32)] * (ITERS - 1 - iteration))
        )
        if iteration + 1 < ITERS:
            basis.append(image / length)
    hess = jnp.stack(columns_h, axis=1)
    gram = jnp.dot(hess.T, hess, precision=top)
    coeffs = small_solve(gram, beta * hess[0])
    update = jnp.zeros_like(field_state)
    for iteration in range(ITERS):
        update = update + coeffs[iteration] * directions[iteration]
    return (update, resid)


ROUNDS = ITERS + 1
COLUMN_SHIFT = 1.0
MESH = pl.DeviceIdType.MESH


def split(value):
    high = value.astype(jnp.bfloat16)
    low = (value - high.astype(jnp.float32)).astype(jnp.bfloat16)
    return high, low


def wave_tables(groups, local_harm):
    harmonics = groups * local_harm
    samples = 2 * harmonics
    waves = np.arange(harmonics).reshape(groups, 1, local_harm)
    moments = np.arange(samples)[:, None, None, None]
    phase = (moments * waves[None] % samples) * (2.0 * np.pi / samples)
    inverse = np.concatenate([np.cos(phase), -np.sin(phase)], axis=2).reshape(samples, -1)
    weights = np.where(waves == 0, 1.0, 2.0) / samples
    weights = np.concatenate([weights, weights], axis=1).reshape(-1)
    forward = (inverse * weights[None]).T
    result = []
    for table in (inverse, forward):
        table = table.astype(np.float32)
        high = table.astype(jnp.bfloat16)
        low = (table - high.astype(np.float32)).astype(jnp.bfloat16)
        result.append(np.concatenate([high, low], axis=0))
    return np.stack(result)


def kernel(
    groups, blocks_count, dims,
    state_hbm, capacity_hbm, shifts_hbm, kinds_hbm, table_hbm, source_hbm, precond_hbm, waves_hbm,
    update_out, resid_out,
    fields, basis, arrived, answer, returned, image, slopes,
    state, capacity, shifts, kinds, table, source, precond, wave_mats, mat_high, mat_low, gram_send, gram_all,
    local_sems, out_send, out_recv, back_send, back_recv, halo_send, halo_recv, gram_ssem, gram_rsem,
):
    local_harm, rows, columns = dims
    own_rows = rows // groups
    pair = 2 * local_harm
    samples = 2 * groups * local_harm
    devices = groups * blocks_count
    place = lax.axis_index("harm")
    node = lax.axis_index("node")
    me = place * blocks_count + node
    inner_groups = 2 if groups % 2 == 0 else 1
    ring = groups // inner_groups
    order = sorted(
        range(1, groups),
        key=lambda step: -min(step // inner_groups, ring - step // inner_groups)
        - (step % inner_groups > 0),
    )

    loads = [
        pltpu.make_async_copy(precond_hbm, precond, local_sems.at[0]),
        pltpu.make_async_copy(waves_hbm, wave_mats, local_sems.at[1]),
        pltpu.make_async_copy(source_hbm, source, local_sems.at[2]),
        pltpu.make_async_copy(capacity_hbm, capacity, local_sems.at[3]),
        pltpu.make_async_copy(shifts_hbm, shifts, local_sems.at[4]),
        pltpu.make_async_copy(kinds_hbm, kinds, local_sems.at[5]),
        pltpu.make_async_copy(table_hbm, table, local_sems.at[6]),
    ]
    first_load = pltpu.make_async_copy(state_hbm, state, local_sems.at[7])
    first_load.start()
    for load in loads:
        load.start()

    barrier = pltpu.get_barrier_semaphore()

    def greet(step, carry):
        other = lax.rem(me + step, devices)
        pl.semaphore_signal(
            barrier,
            inc=1,
            device_id=(other // blocks_count, lax.rem(other, blocks_count)),
            device_id_type=MESH,
        )
        return carry

    lax.fori_loop(1, devices, greet, 0)

    first_load.wait()
    state_flat = state.reshape(2 * local_harm * rows, columns)
    for row in range(rows):
        for part in range(2):
            fields[0, 1 + row, part * local_harm:(part + 1) * local_harm, :] = state_flat[
                pl.ds(part * local_harm * rows + row, local_harm, stride=rows), :
            ]

    @pl.when(node == 0)
    def _():
        for q in range(ROUNDS):
            fields[q, 0] = jnp.zeros((pair, columns), jnp.float32)

    @pl.when(node == blocks_count - 1)
    def _():
        for q in range(ROUNDS):
            fields[q, rows + 1] = jnp.zeros((pair, columns), jnp.float32)

    pl.semaphore_wait(barrier, devices - 1)

    def partner(step):
        outer = lax.rem(place // inner_groups + step // inner_groups, groups // inner_groups)
        return outer * inner_groups + lax.rem(place + step, inner_groups)

    def out_copy(q, row, step):
        dest = partner(step)
        return pltpu.make_async_remote_copy(
            src_ref=fields.at[q, 1 + dest * own_rows + row],
            dst_ref=arrived.at[q, row, place],
            send_sem=out_send.at[q, row, step],
            recv_sem=out_recv.at[q, row, step],
            device_id=(dest, node),
            device_id_type=MESH,
        )

    def back_copy(q, row, step):
        dest = partner(step)
        return pltpu.make_async_remote_copy(
            src_ref=answer.at[q, row, dest],
            dst_ref=returned.at[q, place * own_rows + row],
            send_sem=back_send.at[q, row, step],
            recv_sem=back_recv.at[q, row, step],
            device_id=(dest, node),
            device_id_type=MESH,
        )

    def halo_copy(q, up):
        return pltpu.make_async_remote_copy(
            src_ref=fields.at[q, 1 if up else rows],
            dst_ref=fields.at[q, rows + 1 if up else 0],
            send_sem=halo_send.at[q, up],
            recv_sem=halo_recv.at[q, up],
            device_id=(place, node - 1 if up else node + 1),
            device_id_type=MESH,
        )

    def each(copy, q, row, action):
        for step in order:
            getattr(copy(q, row, step), action)()

    def halo(q, action):
        @pl.when(node > 0)
        def _():
            if action == "start":
                halo_copy(q, 1).start()
            else:
                halo_copy(q, 1).wait_send()
                halo_copy(q, 0).wait_recv()

        @pl.when(node < blocks_count - 1)
        def _():
            if action == "start":
                halo_copy(q, 0).start()
            else:
                halo_copy(q, 0).wait_send()
                halo_copy(q, 1).wait_recv()

    def send_out(q):
        for row in range(own_rows):
            each(out_copy, q, row, "start")
        halo(q, "start")
        arrived[q, :, place] = fields[q, pl.ds(1 + place * own_rows, own_rows)]

    def send_back(q, row, result):
        answer[q, row] = result.reshape(groups, pair, columns)
        each(back_copy, q, row, "start")
        returned[q, place * own_rows + row] = answer[q, row, place]

    def come_back(q):
        for row in range(own_rows):
            each(back_copy, q, row, "wait")

    def transform(which, value):
        high, low = split(value)
        size = samples
        both = jnp.dot(wave_mats[which], high, preferred_element_type=jnp.float32)
        rest = jnp.dot(wave_mats[which, :size], low, preferred_element_type=jnp.float32)
        return both[:size] + (both[size:] + rest)

    def time_of(q, row):
        each(out_copy, q, row, "wait")
        return transform(0, arrived[q, row].reshape(samples, columns))

    harmonic = (place * local_harm + lax.broadcasted_iota(jnp.int32, (local_harm, columns), 0))
    rate = 0.05 * harmonic.astype(jnp.float32)

    def stencil(q):
        halo(q, "wait")

        def row_of(row, carry):
            here = fields[q, 1 + row]
            above = fields[q, row]
            below = fields[q, 2 + row]
            value = 4.0 * here - pltpu.roll(here, 1, 1) - pltpu.roll(here, columns - 1, 1) - below
            amount_here = shifts[row]
            for amount in range(SHIFTS):
                picked = jnp.where(amount_here == amount, 1.0, 0.0)
                moved = above if amount == 0 else pltpu.roll(above, columns - amount, 1)
                value = value - picked * moved
            reactive = rate * capacity[pl.ds(row, 1), :]
            turned = jnp.concatenate(
                [-reactive * here[local_harm:], reactive * here[:local_harm]], axis=0
            )
            image[row] = value + turned
            return carry

        lax.fori_loop(0, rows, row_of, 0, unroll=4)

    def precondition(q):
        given = basis.at[q].reshape(rows * pair, columns)
        taken = fields.at[q + 1].reshape((rows + 2) * pair, columns)
        for k in range(local_harm):
            real = given[pl.ds(k, rows, stride=pair), :]
            imag = given[pl.ds(local_harm + k, rows, stride=pair), :]
            high, low = split(jnp.concatenate([real, imag], axis=1))
            both = jnp.dot(
                jnp.concatenate([high, low], axis=0), mat_high[k], preferred_element_type=jnp.float32
            )
            rest = jnp.dot(high, mat_low[k], preferred_element_type=jnp.float32)
            value = both[:rows] + (both[rows:] + rest)
            taken[pl.ds(pair + k, rows, stride=pair), :] = value[:, :columns]
            taken[pl.ds(pair + local_harm + k, rows, stride=pair), :] = value[:, columns:]

    def inner(first, second):
        total = jnp.zeros((pair, columns), jnp.float32)
        for row in range(rows):
            total = total + basis[first, row] * basis[second, row]
        return jnp.sum(jnp.sum(total, axis=0, keepdims=True), axis=1, keepdims=True)

    send_out(0)

    loads[0].wait()

    def prepare(k, carry):
        real = precond[0, k].T
        imag = precond[1, k].T
        for part, left, right in ((0, real, imag), (1, -imag, real)):
            high, low = split(jnp.concatenate([left, right], axis=1))
            mat_high[k, part * columns:(part + 1) * columns, :] = high
            mat_low[k, part * columns:(part + 1) * columns, :] = low
        return carry

    lax.fori_loop(0, local_harm, prepare, 0)
    for load in loads[1:]:
        load.wait()

    stencil(0)
    for row in range(own_rows):
        kind = kinds[pl.ds(place * own_rows + row, 1), :]
        params = []
        for member in range(3):
            value = jnp.zeros(kind.shape, jnp.float32)
            for which in range(TYPES):
                value = value + jnp.where(kind == which, 1.0, 0.0) * table[member, which]
            params.append(value)
        linear, amplitude, slope = params
        voltage = time_of(0, row)
        bent = jnp.tanh(slope * voltage)
        send_back(0, row, transform(1, linear * voltage + amplitude * bent))
        slopes[row] = linear + amplitude * slope * (1.0 - bent * bent)
    source_flat = source.reshape(2 * local_harm * rows, columns)
    for row in range(rows):
        for part in range(2):
            image[row, part * local_harm:(part + 1) * local_harm, :] -= source_flat[
                pl.ds(part * local_harm * rows + row, local_harm, stride=rows), :
            ]
    come_back(0)
    basis[0] = -(image[...] + returned[0])

    grams = {}
    for q in range(ITERS):
        precondition(q)
        send_out(q + 1)
        if q == 0:
            resid_out[...] = -basis[0]
        for other in range(q + 1):
            grams[other, q] = inner(other, q)
        stencil(q + 1)
        image[...] = image[...] - COLUMN_SHIFT * basis[q]
        for row in range(own_rows):
            send_back(q + 1, row, transform(1, slopes[row] * time_of(q + 1, row)))
        come_back(q + 1)
        basis[q + 1] = image[...] + returned[q + 1]
    for other in range(ITERS + 1):
        grams[other, ITERS] = inner(other, ITERS)

    lane = lax.broadcasted_iota(jnp.int32, (1, 128), 1)
    packed = jnp.zeros((1, 128), jnp.float32)
    names = sorted(grams)
    for at, name in enumerate(names):
        packed = packed + jnp.where(lane == at, grams[name], 0.0)
    gram_send[...] = packed
    gram_all[me] = packed

    def gram_copy(step):
        other = lax.rem(me + step, devices)
        return pltpu.make_async_remote_copy(
            src_ref=gram_send,
            dst_ref=gram_all.at[me],
            send_sem=gram_ssem.at[step],
            recv_sem=gram_rsem.at[step],
            device_id=(other // blocks_count, lax.rem(other, blocks_count)),
            device_id_type=MESH,
        )

    def gram_start(step, carry):
        gram_copy(step).start()
        return carry

    def gram_wait(step, carry):
        gram_copy(step).wait()
        return carry

    lax.fori_loop(1, devices, gram_start, 0)
    lax.fori_loop(1, devices, gram_wait, 0)
    total = jnp.sum(gram_all[...], axis=0)
    full = {}
    for at, name in enumerate(names):
        value = jnp.sum(jnp.where(lane == at, total, 0.0), axis=1, keepdims=True)
        full[name] = full[name[::-1]] = value
    half = {}
    for a in range(ITERS + 1):
        for j in range(ITERS):
            half[a, j] = full[a, j + 1] + COLUMN_SHIFT * full[a, j]
    normal = {}
    for i in range(ITERS):
        for j in range(ITERS):
            normal[i, j] = half[i + 1, j] + COLUMN_SHIFT * half[i, j]
    right = [half[0, j] for j in range(ITERS)]
    lower, diag = {}, []
    for j in range(ITERS):
        value = normal[j, j]
        for m in range(j):
            value = value - lower[j, m] * lower[j, m] * diag[m]
        diag.append(value)
        for i in range(j + 1, ITERS):
            value = normal[i, j]
            for m in range(j):
                value = value - lower[i, m] * lower[j, m] * diag[m]
            lower[i, j] = value / diag[j]
    forward = []
    for j in range(ITERS):
        value = right[j]
        for m in range(j):
            value = value - lower[j, m] * forward[m]
        forward.append(value)
    coeffs = [None] * ITERS
    for j in reversed(range(ITERS)):
        value = forward[j] / diag[j]
        for m in range(j + 1, ITERS):
            value = value - lower[m, j] * coeffs[m]
        coeffs[j] = value
    for row in range(rows):
        value = coeffs[0] * fields[1, 1 + row]
        for j in range(1, ITERS):
            value = value + coeffs[j] * fields[j + 1, 1 + row]
        update_out[row] = value


def fused(state, source, capacity, row_shift, device_type, device_table, precond):
    groups = lax.axis_size("harm")
    blocks_count = lax.axis_size("node")
    _, local_harm, rows, columns = state.shape
    own_rows = rows // groups
    pair = 2 * local_harm
    samples = 2 * groups * local_harm
    devices = groups * blocks_count
    waves = jnp.asarray(wave_tables(groups, local_harm))
    vmem = pl.BlockSpec(memory_space=pltpu.VMEM)
    anywhere = pl.BlockSpec(memory_space=pl.ANY)
    field = (rows, pair, columns)
    f32 = jnp.float32
    dma = pltpu.SemaphoreType.DMA
    update, resid = pl.pallas_call(
        functools.partial(kernel, groups, blocks_count, (local_harm, rows, columns)),
        out_shape=(jax.ShapeDtypeStruct(field, f32),) * 2,
        in_specs=[anywhere] * 8,
        out_specs=(vmem, vmem),
        scratch_shapes=[
            pltpu.VMEM((ROUNDS, rows + 2, pair, columns), f32),
            pltpu.VMEM((ROUNDS,) + field, f32),
            pltpu.VMEM((ROUNDS, own_rows, groups, pair, columns), f32),
            pltpu.VMEM((ROUNDS, own_rows, groups, pair, columns), f32),
            pltpu.VMEM((ROUNDS,) + field, f32),
            pltpu.VMEM(field, f32),
            pltpu.VMEM((own_rows, samples, columns), f32),
            pltpu.VMEM(state.shape, f32),
            pltpu.VMEM(capacity.shape, f32),
            pltpu.SMEM(row_shift.shape, jnp.int32),
            pltpu.VMEM(device_type.shape, jnp.int32),
            pltpu.SMEM(device_table.shape, f32),
            pltpu.VMEM(source.shape, f32),
            pltpu.VMEM(precond.shape, f32),
            pltpu.VMEM(waves.shape, jnp.bfloat16),
            pltpu.VMEM((local_harm, 2 * columns, 2 * columns), jnp.bfloat16),
            pltpu.VMEM((local_harm, 2 * columns, 2 * columns), jnp.bfloat16),
            pltpu.VMEM((1, 128), f32),
            pltpu.VMEM((devices, 1, 128), f32),
            dma((8,)),
            dma((ROUNDS, own_rows, groups)),
            dma((ROUNDS, own_rows, groups)),
            dma((ROUNDS, own_rows, groups)),
            dma((ROUNDS, own_rows, groups)),
            dma((ROUNDS, 2)),
            dma((ROUNDS, 2)),
            dma((devices,)),
            dma((devices,)),
        ],
        compiler_params=pltpu.CompilerParams(
            collective_id=0, has_side_effects=True, vmem_limit_bytes=67043328
        ),
    )(state, capacity, row_shift, device_type, device_table, source, precond, waves)
    return back(update, state.shape), back(resid, state.shape)


def back(value, shape):
    parts, local_harm, rows, columns = shape
    return jnp.transpose(value.reshape(rows, parts, local_harm, columns), (1, 2, 0, 3))


def chosen(*args):
    groups = lax.axis_size("harm")
    _, local_harm, rows, columns = args[0].shape
    if local_harm % 16 or rows % 16 or rows % groups or columns % 128:
        return body(*args)
    return fused(*args)


def solution(mesh):
    return jax.shard_map(
        chosen,
        mesh=mesh,
        in_specs=(
            P(None, "harm", "node", None),
            P(None, "harm", "node", None),
            P("node", None),
            P("node"),
            P("node", None),
            P(),
            P(None, "harm", None, None),
        ),
        out_specs=(P(None, "harm", "node", None), P(None, "harm", "node", None)),
        check_vma=False,
    )
```

```python
import functools

import jax
import jax.numpy as jnp
import numpy as np
from jax import lax
from jax.experimental import pallas as pl
from jax.experimental.pallas import tpu as pltpu
from jax.sharding import PartitionSpec as P

ITERS = 3
TYPES = 4
SHIFTS = 4


omega_step = 0.05
top = lax.Precision.HIGHEST


def extended(cells, sides, width):
    for axis, dim in sides:
        count = lax.axis_size(axis)
        ends = count - 1
        head = lax.slice_in_dim(cells, 0, width, axis=dim)
        tail = lax.slice_in_dim(cells, cells.shape[dim] - width, cells.shape[dim], axis=dim)
        cells = jnp.concatenate(
            [
                lax.ppermute(tail, axis, [(i, (i + 1) % count) for i in range(ends)]),
                cells,
                lax.ppermute(head, axis, [((i + 1) % count, i) for i in range(ends)]),
            ],
            axis=dim,
        )
    return cells


def small_solve(gram, right):
    lower = jnp.linalg.cholesky(gram)
    order = gram.shape[0]
    forward = []
    for column in range(order):
        value = right[column]
        for member in range(column):
            value = value - lower[column, member] * forward[member]
        forward.append(value / lower[column, column])
    result = [None] * order
    for column in reversed(range(order)):
        value = forward[column]
        for member in range(column + 1, order):
            value = value - lower[member, column] * result[member]
        result[column] = value / lower[column, column]
    return result


def tables(harmonics, samples):
    waves = jnp.arange(harmonics, dtype=jnp.int32)
    moments = jnp.arange(samples, dtype=jnp.int32)
    phase = (moments[:, None] * waves[None, :] % samples).astype(jnp.float32) * (
        2.0 * jnp.pi / samples
    )
    cosine = jnp.cos(phase)
    sine = jnp.sin(phase)
    inverse = jnp.concatenate([cosine, -sine], axis=1)
    weights = jnp.where(waves == 0, 1.0, 2.0).astype(jnp.float32) / samples
    forward = jnp.concatenate([cosine.T * weights[:, None], -sine.T * weights[:, None]], axis=0)
    return (inverse, forward)


def stencil(field, above, below, capacity, shifts, waves):
    left_side = jnp.roll(field, 1, axis=3)
    right_side = jnp.roll(field, -1, axis=3)
    skewed = jnp.zeros_like(field)
    for amount in range(SHIFTS):
        picked = (shifts == amount).astype(jnp.float32)[None, None, :, None]
        skewed = skewed + picked * jnp.roll(above, -amount, axis=3)
    result = 4.0 * field - left_side - right_side - skewed - below
    reactive = omega_step * waves.astype(jnp.float32)[:, None, None] * capacity[None]
    return result + jnp.stack([-reactive * field[1], reactive * field[0]])


def precondition(field, blocks):
    real_part = jnp.einsum("krd,kcd->krc", field[0], blocks[0], precision=top) - jnp.einsum(
        "krd,kcd->krc", field[1], blocks[1], precision=top
    )
    imag_part = jnp.einsum("krd,kcd->krc", field[0], blocks[1], precision=top) + jnp.einsum(
        "krd,kcd->krc", field[1], blocks[0], precision=top
    )
    return jnp.stack([real_part, imag_part])


def body(state, source, capacity, row_shift, device_type, device_table, precond):
    groups = lax.axis_size("harm")
    place = lax.axis_index("harm")
    local_harm = state.shape[1]
    block_rows = state.shape[2]
    columns = state.shape[3]
    harmonics = local_harm * groups
    samples = 2 * harmonics
    own_rows = block_rows // groups
    inverse, forward = tables(harmonics, samples)
    kinds = lax.dynamic_slice_in_dim(device_type, place * own_rows, own_rows, 0).reshape(-1)
    params = jnp.zeros((3, kinds.shape[0]), jnp.float32)
    for member in range(TYPES):
        params = (
            params
            + (kinds == member).astype(jnp.float32)[None, :] * device_table[:, member][:, None]
        )
    linear, amplitude, slope = (params[0], params[1], params[2])

    def time_of(spectrum):
        return jnp.dot(
            inverse,
            spectrum.reshape(2 * harmonics, -1),
            precision=top,
            preferred_element_type=jnp.float32,
        )

    def spectrum_of(signal):
        return jnp.dot(forward, signal, precision=top, preferred_element_type=jnp.float32).reshape(
            2, harmonics, own_rows, columns
        )

    def currents(spectrum):
        voltage = time_of(spectrum)
        bent = jnp.tanh(slope * voltage)
        flow = linear * voltage + amplitude * bent
        slopes_now = linear + amplitude * slope * (1.0 - bent * bent)
        return (spectrum_of(flow), slopes_now)

    field_state, field_source = (state, source)
    waves = place * local_harm + jnp.arange(local_harm, dtype=jnp.int32)

    def sides(field):
        padded = extended(field, (("node", 2),), 1)
        return (padded[:, :, :-2], padded[:, :, 2:])

    def across(field, local):
        moved = lax.all_to_all(field, "harm", split_axis=2, concat_axis=1, tiled=True)
        result, extra = local(moved)
        return (lax.all_to_all(result, "harm", split_axis=1, concat_axis=2, tiled=True), extra)

    def operator(field):
        above, below = sides(field)
        return stencil(field, above, below, capacity, row_shift, waves)

    spec_flow, slopes = across(field_state, currents)
    resid = operator(field_state) + spec_flow - field_source

    def linear_part(spectrum):
        return (spectrum_of(slopes * time_of(spectrum)), slopes)

    start = -resid
    beta = jnp.sqrt(lax.psum(jnp.sum(start * start), ("harm", "node")))
    basis = [start / beta]
    directions = []
    columns_h = []
    for iteration in range(ITERS):
        direction = precondition(basis[iteration], precond)
        directions.append(direction)
        coupled, unused = across(direction, linear_part)
        image = operator(direction) + coupled
        locals_dot = jnp.stack([jnp.sum(basis[member] * image) for member in range(iteration + 1)])
        totals, square = lax.psum((locals_dot, jnp.sum(image * image)), ("harm", "node"))
        heights = [totals[member] for member in range(iteration + 1)]
        for earlier in range(iteration + 1):
            image = image - heights[earlier] * basis[earlier]
        length = jnp.sqrt(square - jnp.sum(totals * totals))
        columns_h.append(
            jnp.stack(heights + [length] + [jnp.zeros((), jnp.float32)] * (ITERS - 1 - iteration))
        )
        if iteration + 1 < ITERS:
            basis.append(image / length)
    hess = jnp.stack(columns_h, axis=1)
    gram = jnp.dot(hess.T, hess, precision=top)
    coeffs = small_solve(gram, beta * hess[0])
    update = jnp.zeros_like(field_state)
    for iteration in range(ITERS):
        update = update + coeffs[iteration] * directions[iteration]
    return (update, resid)


ROUNDS = ITERS + 1
COLUMN_SHIFT = 1.0
MESH = pl.DeviceIdType.MESH


def split(value):
    high = value.astype(jnp.bfloat16)
    low = (value - high.astype(jnp.float32)).astype(jnp.bfloat16)
    return high, low


def wave_tables(groups, local_harm):
    harmonics = groups * local_harm
    samples = 2 * harmonics
    waves = np.arange(harmonics).reshape(groups, 1, local_harm)
    moments = np.arange(samples)[:, None, None, None]
    phase = (moments * waves[None] % samples) * (2.0 * np.pi / samples)
    inverse = np.concatenate([np.cos(phase), -np.sin(phase)], axis=2).reshape(samples, -1)
    weights = np.where(waves == 0, 1.0, 2.0) / samples
    weights = np.concatenate([weights, weights], axis=1).reshape(-1)
    forward = (inverse * weights[None]).T
    result = []
    for table in (inverse, forward):
        table = table.astype(np.float32)
        high = table.astype(jnp.bfloat16)
        low = (table - high.astype(np.float32)).astype(jnp.bfloat16)
        result.append(np.concatenate([high, low], axis=0))
    return np.stack(result)


def kernel(
    groups, blocks_count, dims,
    state_hbm, capacity_hbm, shifts_hbm, kinds_hbm, table_hbm, source_hbm, precond_hbm, waves_hbm,
    update_out, resid_out,
    fields, basis, arrived, answer, returned, image, slopes,
    resid_stage, state, capacity, shifts, kinds, table, source, precond, wave_mats, mat_high, mat_low, gram_send, gram_all,
    local_sems, out_send, out_recv, back_send, back_recv, halo_send, halo_recv, gram_ssem, gram_rsem,
):
    local_harm, rows, columns = dims
    own_rows = rows // groups
    pair = 2 * local_harm
    samples = 2 * groups * local_harm
    devices = groups * blocks_count
    place = lax.axis_index("harm")
    node = lax.axis_index("node")
    me = place * blocks_count + node
    inner_groups = 2 if groups % 2 == 0 else 1
    ring = groups // inner_groups
    order = sorted(
        range(1, groups),
        key=lambda step: -min(step // inner_groups, ring - step // inner_groups)
        - (step % inner_groups > 0),
    )

    loads = [
        pltpu.make_async_copy(precond_hbm, precond, local_sems.at[0]),
        pltpu.make_async_copy(waves_hbm, wave_mats, local_sems.at[1]),
        pltpu.make_async_copy(source_hbm, source, local_sems.at[2]),
        pltpu.make_async_copy(capacity_hbm, capacity, local_sems.at[3]),
        pltpu.make_async_copy(shifts_hbm, shifts, local_sems.at[4]),
        pltpu.make_async_copy(kinds_hbm, kinds, local_sems.at[5]),
        pltpu.make_async_copy(table_hbm, table, local_sems.at[6]),
    ]
    first_load = pltpu.make_async_copy(state_hbm, state, local_sems.at[7])
    first_load.start()
    resid_store = pltpu.make_async_copy(resid_stage, resid_out, local_sems.at[8])
    for load in loads:
        load.start()

    barrier = pltpu.get_barrier_semaphore()

    harm_places = [lax.rem(place + step, groups) for step in range(groups)]
    node_places = [lax.rem(node + step, blocks_count) for step in range(blocks_count)]
    others = [(a, b) for a in range(groups) for b in range(blocks_count) if a + b > 0]
    for a, b in others:
        pl.semaphore_signal(
            barrier,
            inc=1,
            device_id=(harm_places[a], node_places[b]),
            device_id_type=MESH,
        )

    first_load.wait()
    state_flat = state.reshape(2 * local_harm * rows, columns)
    for row in range(rows):
        for part in range(2):
            fields[0, 1 + row, part * local_harm:(part + 1) * local_harm, :] = state_flat[
                pl.ds(part * local_harm * rows + row, local_harm, stride=rows), :
            ]

    @pl.when(node == 0)
    def _():
        for q in range(ROUNDS):
            fields[q, 0] = jnp.zeros((pair, columns), jnp.float32)

    @pl.when(node == blocks_count - 1)
    def _():
        for q in range(ROUNDS):
            fields[q, rows + 1] = jnp.zeros((pair, columns), jnp.float32)

    pl.semaphore_wait(barrier, devices - 1)

    def partner(step):
        outer = lax.rem(place // inner_groups + step // inner_groups, groups // inner_groups)
        return outer * inner_groups + lax.rem(place + step, inner_groups)

    def out_copy(q, row, step):
        dest = partner(step)
        return pltpu.make_async_remote_copy(
            src_ref=fields.at[q, 1 + dest * own_rows + row],
            dst_ref=arrived.at[q, row, place],
            send_sem=out_send.at[q, row, step],
            recv_sem=out_recv.at[q, row, step],
            device_id=(dest, node),
            device_id_type=MESH,
        )

    def back_copy(q, row, step):
        dest = partner(step)
        return pltpu.make_async_remote_copy(
            src_ref=answer.at[q, row, dest],
            dst_ref=returned.at[q, place * own_rows + row],
            send_sem=back_send.at[q, row, step],
            recv_sem=back_recv.at[q, row, step],
            device_id=(dest, node),
            device_id_type=MESH,
        )

    def halo_copy(q, up):
        return pltpu.make_async_remote_copy(
            src_ref=fields.at[q, 1 if up else rows],
            dst_ref=fields.at[q, rows + 1 if up else 0],
            send_sem=halo_send.at[q, up],
            recv_sem=halo_recv.at[q, up],
            device_id=(place, node - 1 if up else node + 1),
            device_id_type=MESH,
        )

    def each(copy, q, row, action):
        for step in order:
            getattr(copy(q, row, step), action)()

    def halo(q, action):
        @pl.when(node > 0)
        def _():
            if action == "start":
                halo_copy(q, 1).start()
            else:
                halo_copy(q, 1).wait_send()
                halo_copy(q, 0).wait_recv()

        @pl.when(node < blocks_count - 1)
        def _():
            if action == "start":
                halo_copy(q, 0).start()
            else:
                halo_copy(q, 0).wait_send()
                halo_copy(q, 1).wait_recv()

    def send_out(q):
        halo(q, "start")
        for row in range(own_rows):
            each(out_copy, q, row, "start")
        arrived[q, :, place] = fields[q, pl.ds(1 + place * own_rows, own_rows)]

    def send_back(q, row, result):
        answer[q, row] = result.reshape(groups, pair, columns)
        each(back_copy, q, row, "start")
        returned[q, place * own_rows + row] = answer[q, row, place]

    def come_back(q):
        for row in range(own_rows):
            each(back_copy, q, row, "wait")

    def transform(which, value):
        high, low = split(value)
        size = samples
        both = jnp.dot(wave_mats[which], high, preferred_element_type=jnp.float32)
        rest = jnp.dot(wave_mats[which, :size], low, preferred_element_type=jnp.float32)
        return both[:size] + (both[size:] + rest)

    def time_of(q, row):
        each(out_copy, q, row, "wait")
        return transform(0, arrived[q, row].reshape(samples, columns))

    harmonic = (place * local_harm + lax.broadcasted_iota(jnp.int32, (local_harm, columns), 0))
    rate = 0.05 * harmonic.astype(jnp.float32)

    def stencil(q):
        halo(q, "wait")

        def row_of(row, carry):
            here = fields[q, 1 + row]
            above = fields[q, row]
            below = fields[q, 2 + row]
            value = 4.0 * here - pltpu.roll(here, 1, 1) - pltpu.roll(here, columns - 1, 1) - below
            amount_here = shifts[row]
            for amount in range(SHIFTS):
                picked = jnp.where(amount_here == amount, 1.0, 0.0)
                moved = above if amount == 0 else pltpu.roll(above, columns - amount, 1)
                value = value - picked * moved
            reactive = rate * capacity[pl.ds(row, 1), :]
            turned = jnp.concatenate(
                [-reactive * here[local_harm:], reactive * here[:local_harm]], axis=0
            )
            image[row] = value + turned
            return carry

        lax.fori_loop(0, rows, row_of, 0, unroll=4)

    def precondition(q):
        given = basis.at[q].reshape(rows * pair, columns)
        taken = fields.at[q + 1].reshape((rows + 2) * pair, columns)
        for k in range(local_harm):
            real = given[pl.ds(k, rows, stride=pair), :]
            imag = given[pl.ds(local_harm + k, rows, stride=pair), :]
            high, low = split(jnp.concatenate([real, imag], axis=1))
            both = jnp.dot(
                jnp.concatenate([high, low], axis=0), mat_high[k], preferred_element_type=jnp.float32
            )
            rest = jnp.dot(high, mat_low[k], preferred_element_type=jnp.float32)
            value = both[:rows] + (both[rows:] + rest)
            taken[pl.ds(pair + k, rows, stride=pair), :] = value[:, :columns]
            taken[pl.ds(pair + local_harm + k, rows, stride=pair), :] = value[:, columns:]

    def inner(first, second):
        total = jnp.zeros((pair, columns), jnp.float32)
        for row in range(rows):
            total = total + basis[first, row] * basis[second, row]
        return jnp.sum(jnp.sum(total, axis=0, keepdims=True), axis=1, keepdims=True)

    send_out(0)

    loads[0].wait()

    def prepare(k, carry):
        real = precond[0, k].T
        imag = precond[1, k].T
        for part, left, right in ((0, real, imag), (1, -imag, real)):
            high, low = split(jnp.concatenate([left, right], axis=1))
            mat_high[k, part * columns:(part + 1) * columns, :] = high
            mat_low[k, part * columns:(part + 1) * columns, :] = low
        return carry

    lax.fori_loop(0, local_harm, prepare, 0)
    for load in loads[1:]:
        load.wait()

    for row in range(own_rows):
        kind = kinds[pl.ds(place * own_rows + row, 1), :]
        params = []
        for member in range(3):
            value = jnp.zeros(kind.shape, jnp.float32)
            for which in range(TYPES):
                value = value + jnp.where(kind == which, 1.0, 0.0) * table[member, which]
            params.append(value)
        linear, amplitude, slope = params
        voltage = time_of(0, row)
        bent = jnp.tanh(slope * voltage)
        send_back(0, row, transform(1, linear * voltage + amplitude * bent))
        slopes[row] = linear + amplitude * slope * (1.0 - bent * bent)
    stencil(0)
    source_flat = source.reshape(2 * local_harm * rows, columns)
    for row in range(rows):
        for part in range(2):
            image[row, part * local_harm:(part + 1) * local_harm, :] -= source_flat[
                pl.ds(part * local_harm * rows + row, local_harm, stride=rows), :
            ]
    come_back(0)
    basis[0] = -(image[...] + returned[0])

    grams = {}
    for q in range(ITERS):
        precondition(q)
        send_out(q + 1)
        if q == 0:
            resid_stage[...] = -basis[0]
            resid_store.start()
        for other in range(q + 1):
            grams[other, q] = inner(other, q)
        for row in range(own_rows):
            send_back(q + 1, row, transform(1, slopes[row] * time_of(q + 1, row)))
        stencil(q + 1)
        image[...] = image[...] - COLUMN_SHIFT * basis[q]
        come_back(q + 1)
        basis[q + 1] = image[...] + returned[q + 1]
    for other in range(ITERS + 1):
        grams[other, ITERS] = inner(other, ITERS)

    lane = lax.broadcasted_iota(jnp.int32, (1, 128), 1)
    packed = jnp.zeros((1, 128), jnp.float32)
    names = sorted(grams)
    for at, name in enumerate(names):
        packed = packed + jnp.where(lane == at, grams[name], 0.0)
    gram_send[...] = packed
    gram_all[me] = packed

    copies = [
        pltpu.make_async_remote_copy(
            src_ref=gram_send,
            dst_ref=gram_all.at[me],
            send_sem=gram_ssem.at[a * blocks_count + b],
            recv_sem=gram_rsem.at[a * blocks_count + b],
            device_id=(harm_places[a], node_places[b]),
            device_id_type=MESH,
        )
        for a, b in others
    ]
    for copy in copies:
        copy.start()
    for copy in copies:
        copy.wait()
    total = jnp.sum(gram_all[...], axis=0)
    full = {}
    for at, name in enumerate(names):
        value = jnp.sum(jnp.where(lane == at, total, 0.0), axis=1, keepdims=True)
        full[name] = full[name[::-1]] = value
    half = {}
    for a in range(ITERS + 1):
        for j in range(ITERS):
            half[a, j] = full[a, j + 1] + COLUMN_SHIFT * full[a, j]
    normal = {}
    for i in range(ITERS):
        for j in range(ITERS):
            normal[i, j] = half[i + 1, j] + COLUMN_SHIFT * half[i, j]
    right = [half[0, j] for j in range(ITERS)]
    lower, diag = {}, []
    for j in range(ITERS):
        value = normal[j, j]
        for m in range(j):
            value = value - lower[j, m] * lower[j, m] * diag[m]
        diag.append(value)
        for i in range(j + 1, ITERS):
            value = normal[i, j]
            for m in range(j):
                value = value - lower[i, m] * lower[j, m] * diag[m]
            lower[i, j] = value / diag[j]
    forward = []
    for j in range(ITERS):
        value = right[j]
        for m in range(j):
            value = value - lower[j, m] * forward[m]
        forward.append(value)
    coeffs = [None] * ITERS
    for j in reversed(range(ITERS)):
        value = forward[j] / diag[j]
        for m in range(j + 1, ITERS):
            value = value - lower[m, j] * coeffs[m]
        coeffs[j] = value
    for row in range(rows):
        value = coeffs[0] * fields[1, 1 + row]
        for j in range(1, ITERS):
            value = value + coeffs[j] * fields[j + 1, 1 + row]
        update_out[row] = value
    resid_store.wait()


def fused(state, source, capacity, row_shift, device_type, device_table, precond):
    groups = lax.axis_size("harm")
    blocks_count = lax.axis_size("node")
    _, local_harm, rows, columns = state.shape
    own_rows = rows // groups
    pair = 2 * local_harm
    samples = 2 * groups * local_harm
    devices = groups * blocks_count
    waves = jnp.asarray(wave_tables(groups, local_harm))
    vmem = pl.BlockSpec(memory_space=pltpu.VMEM)
    anywhere = pl.BlockSpec(memory_space=pl.ANY)
    field = (rows, pair, columns)
    f32 = jnp.float32
    dma = pltpu.SemaphoreType.DMA
    update, resid = pl.pallas_call(
        functools.partial(kernel, groups, blocks_count, (local_harm, rows, columns)),
        out_shape=(jax.ShapeDtypeStruct(field, f32),) * 2,
        in_specs=[anywhere] * 8,
        out_specs=(vmem, anywhere),
        scratch_shapes=[
            pltpu.VMEM((ROUNDS, rows + 2, pair, columns), f32),
            pltpu.VMEM((ROUNDS,) + field, f32),
            pltpu.VMEM((ROUNDS, own_rows, groups, pair, columns), f32),
            pltpu.VMEM((ROUNDS, own_rows, groups, pair, columns), f32),
            pltpu.VMEM((ROUNDS,) + field, f32),
            pltpu.VMEM(field, f32),
            pltpu.VMEM((own_rows, samples, columns), f32),
            pltpu.VMEM(field, f32),
            pltpu.VMEM(state.shape, f32),
            pltpu.VMEM(capacity.shape, f32),
            pltpu.SMEM(row_shift.shape, jnp.int32),
            pltpu.VMEM(device_type.shape, jnp.int32),
            pltpu.SMEM(device_table.shape, f32),
            pltpu.VMEM(source.shape, f32),
            pltpu.VMEM(precond.shape, f32),
            pltpu.VMEM(waves.shape, jnp.bfloat16),
            pltpu.VMEM((local_harm, 2 * columns, 2 * columns), jnp.bfloat16),
            pltpu.VMEM((local_harm, 2 * columns, 2 * columns), jnp.bfloat16),
            pltpu.VMEM((1, 128), f32),
            pltpu.VMEM((devices, 1, 128), f32),
            dma((9,)),
            dma((ROUNDS, own_rows, groups)),
            dma((ROUNDS, own_rows, groups)),
            dma((ROUNDS, own_rows, groups)),
            dma((ROUNDS, own_rows, groups)),
            dma((ROUNDS, 2)),
            dma((ROUNDS, 2)),
            dma((devices,)),
            dma((devices,)),
        ],
        compiler_params=pltpu.CompilerParams(
            collective_id=0, has_side_effects=True, vmem_limit_bytes=67043328
        ),
    )(state, capacity, row_shift, device_type, device_table, source, precond, waves)
    return back(update, state.shape), back(resid, state.shape)


def back(value, shape):
    parts, local_harm, rows, columns = shape
    return jnp.transpose(value.reshape(rows, parts, local_harm, columns), (1, 2, 0, 3))


def chosen(*args):
    groups = lax.axis_size("harm")
    _, local_harm, rows, columns = args[0].shape
    if local_harm % 16 or rows % 16 or rows % groups or columns % 128:
        return body(*args)
    return fused(*args)


def solution(mesh):
    return jax.shard_map(
        chosen,
        mesh=mesh,
        in_specs=(
            P(None, "harm", "node", None),
            P(None, "harm", "node", None),
            P("node", None),
            P("node"),
            P("node", None),
            P(),
            P(None, "harm", None, None),
        ),
        out_specs=(P(None, "harm", "node", None), P(None, "harm", "node", None)),
        check_vma=False,
    )
```
